32 devices in a mesh: dp: 16 (over z, y, x), tensor: 2 (over core).
Axes of the slice: x: 2, y: 2, z: 4, core: 2. Of those that a mesh axis runs over, the one named last changes fastest.
Arguments:
- tokens: bfloat16 [25088, 1024], P('dp'), may hold values from -6 to 6
- attention_gain: float32 [1024], replicated, may hold values from 0.25 to 1.75
- attention_shift: float32 [1024], replicated, may hold values from -3 to 3
- input_weight: bfloat16 [1024, 3, 1024], P(None, None, 'tensor'), may hold values from -0.1875 to 0.1875
- query_bias: float32 [1024], P('tensor'), may hold values from -3 to 3
- value_bias: float32 [1024], P('tensor'), may hold values from -3 to 3
- output_weight: bfloat16 [1024, 1024], P('tensor'), may hold values from -1.5 to 1.5
- output_bias: float32 [1024], replicated, may hold values from -3 to 3
- feedforward_gain: float32 [1024], replicated, may hold values from 0.25 to 1.75
- feedforward_shift: float32 [1024], replicated, may hold values from -3 to 3
- expand_weight: bfloat16 [1024, 4096], P(None, 'tensor'), may hold values from -0.1875 to 0.1875
- expand_bias: float32 [4096], P('tensor'), may hold values from -3 to 3
- reduce_weight: bfloat16 [4096, 1024], P('tensor'), may hold values from -0.09375 to 0.09375
- reduce_bias: float32 [1024], replicated, may hold values from -3 to 3
- cotangent: bfloat16 [25088, 1024], P('dp'), may hold values from -6 to 6
Outputs:
- block_out: bfloat16 [25088, 1024], P('dp')
- tokens_gradient: bfloat16 [25088, 1024], P('dp')
- attention_gain_gradient: float32 [1024], replicated
- attention_shift_gradient: float32 [1024], replicated
- input_weight_gradient: float32 [1024, 3, 1024], P(None, None, 'tensor')
- query_bias_gradient: float32 [1024], P('tensor')
- value_bias_gradient: float32 [1024], P('tensor')
- output_weight_gradient: float32 [1024, 1024], P('tensor')
- output_bias_gradient: float32 [1024], replicated
- feedforward_gain_gradient: float32 [1024], replicated
- feedforward_shift_gradient: float32 [1024], replicated
- expand_weight_gradient: float32 [1024, 4096], P(None, 'tensor')
- expand_bias_gradient: float32 [4096], P('tensor')
- reduce_weight_gradient: float32 [4096, 1024], P('tensor')
- reduce_bias_gradient: float32 [1024], replicated
The draws below stay inside these ranges and needn't reach their ends.
All inputs are finite; a program needn't handle non-finite values.
Results may differ from the reference program's by a relative error of at most 0.013.
The reference program's roundings to bfloat16 on the way count: a program that leaves them out, or rounds other values in their place, can miss the bound.
Values may be sent and summed in bfloat16 or wider, within the bound.
A program may use at most 384 MiB of HBM per device.

```python
import jax
import jax.numpy as jnp
from jax import lax

D = 1024
HEADS = 16
HEAD_DIM = 64
FF = 4096
SEQ = 1568
TOKENS = 25088


def block_levels(stream_key, shape, cuts, low, top_value):
    def one(axis_at, blocks):
        steps = jax.random.uniform(jax.random.fold_in(jax.random.fold_in(stream_key, 6), axis_at), (blocks,), jnp.float32, low / len(cuts), top_value / len(cuts))
        return jnp.repeat(jnp.exp(steps), shape[axis_at] // blocks).reshape((-1,) + (1,) * (len(shape) - axis_at - 1))

    loudness = one(*cuts[0])
    for cut in cuts[1:]:
        loudness = loudness * one(*cut)
    return loudness


def centred(stream_key, extent, scale, reach, split=(), held_as=jnp.bfloat16):
    array = jax.random.normal(stream_key, extent, jnp.float32) * scale
    if len(split) > 0:
        array = block_levels(stream_key, extent, split, -0.22, 0.18) * array
    return jnp.clip(array, min=-reach, max=reach).astype(held_as)


def setup_inputs(seed: int = 0) -> dict:
    splits = jax.random.split(jax.random.key(seed), 16)
    return {
        "tokens": centred(splits[0], (TOKENS, D), 1.0, 6.0, ((0, 16),)),
        "attention_gain": jnp.clip(1.0 + 0.15 * jax.random.normal(splits[1], (D,), jnp.float32), 0.25, 1.75),
        "attention_shift": centred(splits[2], (D,), 0.5, 3.0, (), jnp.float32),
        "input_weight": centred(splits[3], (D, 3, D), D ** -0.5, 0.1875, ((2, 2),)),
        "query_bias": centred(splits[4], (D,), 0.5, 3.0, ((0, 2),), jnp.float32),
        "value_bias": centred(splits[5], (D,), 0.5, 3.0, ((0, 2),), jnp.float32),
        "output_weight": centred(splits[6], (D, D), (D // 64) ** -0.5, 1.5, ((0, 2),)),
        "output_bias": centred(splits[7], (D,), 0.5, 3.0, (), jnp.float32),
        "feedforward_gain": jnp.clip(1.0 + 0.15 * jax.random.normal(splits[8], (D,), jnp.float32), 0.25, 1.75),
        "feedforward_shift": centred(splits[9], (D,), 0.5, 3.0, (), jnp.float32),
        "expand_weight": centred(splits[10], (D, FF), D ** -0.5, 0.1875, ((1, 2),)),
        "expand_bias": centred(splits[11], (FF,), 0.5, 3.0, ((0, 2),), jnp.float32),
        "reduce_weight": centred(splits[12], (FF, D), FF ** -0.5, 0.09375, ((0, 2),)),
        "reduce_bias": centred(splits[13], (D,), 0.5, 3.0, (), jnp.float32),
        "cotangent": centred(splits[14], (TOKENS, D), 1.0, 6.0, ((0, 16),)),
    }


norm_eps = 1e-06
highest = lax.Precision.HIGHEST

@jax.custom_vjp
def low(v):
    return lax.optimization_barrier(v.astype(jnp.bfloat16)).astype(jnp.float32)

@jax.custom_vjp
def low_back(v):
    return v

def low_keep(v):
    return (low(v), None)

def low_pass(kept, grad):
    return (grad,)

def back_keep(v):
    return (v, None)

def back_low(kept, grad):
    return (low(grad),)
low.defvjp(low_keep, low_pass)
low_back.defvjp(back_keep, back_low)

def layer_norm(values, gain, shift):
    center = values - lax.optimization_barrier(jnp.mean(values, axis=-1, keepdims=True))
    spread = lax.optimization_barrier(jnp.mean(center * center, axis=-1, keepdims=True))
    return center * lax.rsqrt(spread + norm_eps) * gain + shift

def matmul(left, right):
    return jnp.dot(left, right, precision=highest, preferred_element_type=jnp.float32)

def clip_forward(inputs, attention_gain, attention_shift, input_weight, query_bias, value_bias, output_weight, output_bias, feedforward_gain, feedforward_shift, expand_weight, expand_bias, reduce_weight, reduce_bias):
    normed = low(layer_norm(inputs, attention_gain, attention_shift))
    joint = jnp.einsum('td,dcf->tcf', normed, input_weight, precision=highest)
    joint_bias = jnp.stack([query_bias, jnp.zeros_like(query_bias), value_bias])
    joint = low(low_back(joint + joint_bias))
    heads = joint.reshape(SEQ, 3, HEADS, HEAD_DIM)
    queries = heads[:, 0].reshape(2, SEQ // 2, HEADS, HEAD_DIM)
    keys_all = heads[:, 1]
    values_all = heads[:, 2]
    factor = HEAD_DIM ** (-0.5)

    def attend(query_block):
        scores = low_back(jnp.einsum('qhe,khe->hqk', query_block, keys_all, precision=highest) * factor)
        top = lax.optimization_barrier(jnp.max(scores, axis=-1, keepdims=True))
        weights = jnp.exp(scores - top)
        chances = weights / lax.optimization_barrier(jnp.sum(weights, axis=-1, keepdims=True))
        return jnp.einsum('hqk,khe->qhe', low(chances), values_all, precision=highest)
    mixed = lax.map(jax.checkpoint(attend), queries).reshape(SEQ, HEADS * HEAD_DIM)
    attended = low(low_back(mixed))
    branch = low_back(matmul(attended, output_weight) + output_bias)
    middle = inputs + branch
    normed_two = low(layer_norm(middle, feedforward_gain, feedforward_shift))
    hidden = low_back(matmul(normed_two, expand_weight) + expand_bias)
    activated = low(jax.nn.gelu(hidden, approximate=False))
    update = low_back(matmul(activated, reduce_weight) + reduce_bias)
    return middle + update

def reference(tokens, attention_gain, attention_shift, input_weight, query_bias, value_bias, output_weight, output_bias, feedforward_gain, feedforward_shift, expand_weight, expand_bias, reduce_weight, reduce_bias, cotangent):
    parameters = tuple((p.astype(jnp.float32) for p in (attention_gain, attention_shift, input_weight, query_bias, value_bias, output_weight, output_bias, feedforward_gain, feedforward_shift, expand_weight, expand_bias, reduce_weight, reduce_bias)))
    clips_in = tokens.astype(jnp.float32).reshape(-1, SEQ, D)
    clips_back = cotangent.astype(jnp.float32).reshape(-1, SEQ, D)

    def step(totals, item):
        inputs, upstream = item
        result, pull = jax.vjp(clip_forward, inputs, *parameters)
        gradients = pull(upstream)
        totals = tuple((a + b for a, b in zip(totals, gradients[1:])))
        return (totals, (result.astype(jnp.bfloat16), gradients[0].astype(jnp.bfloat16)))
    start = tuple((jnp.zeros_like(p) for p in parameters))
    totals, (outputs, input_grads) = lax.scan(step, start, (clips_in, clips_back))
    return (outputs.reshape(-1, D), input_grads.reshape(-1, D), totals[0], totals[1], totals[2], totals[3], totals[4], totals[5], totals[6], totals[7], totals[8], totals[9], totals[10], totals[11], totals[12])
```

```python
import functools

import jax
import jax.numpy as jnp
from jax import lax
from jax.experimental import pallas as pl
from jax.experimental.pallas import tpu as pltpu
from jax.sharding import PartitionSpec as P

HEAD_DIM = 64
SEQ = 1568
PAIR = 2 * HEAD_DIM
F32 = jnp.float32
BF16 = jnp.bfloat16
EXP_SCALE = 0.125 * 1.4426950408889634

norm_eps = 1e-06


def layer_norm(values, gain, shift):
    center = values - jnp.mean(values, axis=-1, keepdims=True)
    spread = jnp.mean(center * center, axis=-1, keepdims=True)
    return center * lax.rsqrt(spread + norm_eps) * gain + shift


def exact_gelu(values):
    return jax.nn.gelu(values, approximate=False)


def dot_nn(a, b):
    return lax.dot_general(a, b, (((1,), (0,)), ((), ())), preferred_element_type=F32)


def dot_nt(a, b):
    return lax.dot_general(a, b, (((1,), (1,)), ((), ())), preferred_element_type=F32)


def dot_tn(a, b):
    return lax.dot_general(a, b, (((0,), (0,)), ((), ())), preferred_element_type=F32)


def attend_kernel(q_ref, k_ref, v_ref, out_ref, inverse_ref, weights_ref):
    low_half = lax.broadcasted_iota(jnp.int32, (1, PAIR), 1) < HEAD_DIM
    zero = jnp.zeros((), BF16)
    keys, values, queries = k_ref[...], v_ref[...], q_ref[...]
    mixed, inverses = [], []
    for head in range(2):
        own_keys = jnp.where(low_half if head == 0 else ~low_half, keys, zero)
        scores = dot_nt(queries, own_keys)
        top = jnp.max(scores, axis=1, keepdims=True)
        weights = jnp.exp2((scores - top) * EXP_SCALE)
        inverse = 1.0 / jnp.sum(weights, axis=1, keepdims=True)
        weights = weights.astype(BF16)
        weights_ref[head] = weights
        mixed.append(dot_nn(weights, values) * inverse)
        inverses.append(inverse)
    out_ref[...] = jnp.where(low_half, mixed[0], mixed[1]).astype(BF16)
    inverse_ref[...] = jnp.where(low_half, inverses[0], inverses[1])


def attend(queries, keys, values, block=224):
    rows, width = queries.shape
    pairs = width // PAIR
    tile = pl.BlockSpec((block, PAIR), lambda p, i: (i, p))
    whole = pl.BlockSpec((rows, PAIR), lambda p, i: (0, p))
    return pl.pallas_call(
        attend_kernel,
        grid=(pairs, rows // block),
        in_specs=[tile, whole, whole],
        out_specs=[tile, tile, pl.BlockSpec((2, block, rows), lambda p, i: (p, i, 0))],
        out_shape=[
            jax.ShapeDtypeStruct((rows, width), BF16),
            jax.ShapeDtypeStruct((rows, width), F32),
            jax.ShapeDtypeStruct((2 * pairs, rows, rows), BF16),
        ],
        compiler_params=pltpu.CompilerParams(vmem_limit_bytes=60 << 20),
        cost_estimate=pl.CostEstimate(
            flops=8 * pairs * rows * rows * HEAD_DIM * 4,
            bytes_accessed=4 * pairs * rows * rows,
            transcendentals=2 * pairs * rows * rows,
        ),
        name="attend",
    )(queries, keys, values)


def attend_back_kernel(
    q_ref, k_ref, v_ref, g_ref, o_ref, inverse_ref, weights_ref, dq_ref, dk_ref, dv_ref, dk_sum, dv_sum
):
    step, steps = pl.program_id(1), pl.num_programs(1)
    low_half = lax.broadcasted_iota(jnp.int32, (1, PAIR), 1) < HEAD_DIM
    zero = jnp.zeros((), BF16)

    @pl.when(step == 0)
    def _():
        dk_sum[...] = jnp.zeros_like(dk_sum)
        dv_sum[...] = jnp.zeros_like(dv_sum)

    keys, values, queries = k_ref[...], v_ref[...], q_ref[...]
    grads = (g_ref[...].astype(F32) * inverse_ref[...]).astype(BF16)
    products = grads.astype(F32) * o_ref[...].astype(F32)
    query_grad = None
    for head in range(2):
        own = low_half if head == 0 else ~low_half
        inner = jnp.sum(jnp.where(own, products, 0.0), axis=1, keepdims=True)
        weights = weights_ref[head]
        pushed = dot_nt(grads, jnp.where(own, values, zero))
        score_grad = (weights.astype(F32) * (pushed - inner)).astype(BF16)
        part = dot_nn(score_grad, jnp.where(own, keys, zero))
        query_grad = part if query_grad is None else query_grad + part
        dv_sum[...] += dot_tn(weights, jnp.where(own, grads, zero))
        dk_sum[...] += dot_tn(score_grad, jnp.where(own, queries, zero))
    dq_ref[...] = (query_grad * 0.125).astype(BF16)

    @pl.when(step == steps - 1)
    def _():
        dk_ref[...] = (dk_sum[...] * 0.125).astype(BF16)
        dv_ref[...] = dv_sum[...].astype(BF16)


def attend_back(queries, keys, values, grads, outs, inverse, weights, block=224):
    rows, width = queries.shape
    pairs = width // PAIR
    tile = pl.BlockSpec((block, PAIR), lambda p, i: (i, p))
    whole = pl.BlockSpec((rows, PAIR), lambda p, i: (0, p))
    return pl.pallas_call(
        attend_back_kernel,
        grid=(pairs, rows // block),
        in_specs=[tile, whole, whole, tile, tile, tile, pl.BlockSpec((2, block, rows), lambda p, i: (p, i, 0))],
        out_specs=[tile, whole, whole],
        out_shape=[jax.ShapeDtypeStruct((rows, width), BF16)] * 3,
        scratch_shapes=[pltpu.VMEM((rows, PAIR), F32)] * 2,
        compiler_params=pltpu.CompilerParams(vmem_limit_bytes=60 << 20),
        cost_estimate=pl.CostEstimate(
            flops=16 * pairs * rows * rows * HEAD_DIM * 4,
            bytes_accessed=4 * pairs * rows * rows,
            transcendentals=0,
        ),
        name="attend_back",
    )(queries, keys, values, grads, outs, inverse, weights)


def column_sum(values):
    return jnp.sum(values, axis=0, dtype=F32)


def shards(
    tokens,
    attention_gain,
    attention_shift,
    input_weight,
    query_bias,
    value_bias,
    output_weight,
    output_bias,
    feedforward_gain,
    feedforward_shift,
    expand_weight,
    expand_bias,
    reduce_weight,
    reduce_bias,
    cotangent,
):
    rows = tokens.shape[0]
    share = rows // lax.axis_size("tensor")
    first_row = lax.axis_index("tensor") * share

    def scatter(values):
        return lax.psum_scatter(values, "tensor", scatter_dimension=0, tiled=True)

    def gather(values):
        return lax.all_gather(values, "tensor", axis=0, tiled=True)

    stacked_weight = jnp.transpose(input_weight, (1, 0, 2))
    inputs = tokens.astype(F32)
    upstream = cotangent.astype(F32)
    normed = layer_norm(inputs, attention_gain, attention_shift).astype(BF16)
    queries = (dot_nn(normed, stacked_weight[0]) + query_bias).astype(BF16)
    keys = dot_nn(normed, stacked_weight[1]).astype(BF16)
    values = (dot_nn(normed, stacked_weight[2]) + value_bias).astype(BF16)
    attended, inverse, weights = attend(queries, keys, values)
    own_inputs = lax.dynamic_slice_in_dim(inputs, first_row, share, 0)
    middle = own_inputs + scatter(dot_nn(attended, output_weight).astype(BF16)).astype(F32) + output_bias
    normed_two = layer_norm(middle, feedforward_gain, feedforward_shift).astype(BF16)
    gathered = gather(normed_two)
    hidden = dot_nn(gathered, expand_weight) + expand_bias
    activated = exact_gelu(hidden).astype(BF16)
    result = middle + (scatter(dot_nn(activated, reduce_weight).astype(BF16)).astype(F32) + reduce_bias)
    block_out = gather(result.astype(BF16))
    reduce_bias_grad = column_sum(upstream)
    reduce_weight_grad = dot_tn(activated, cotangent).astype(BF16)
    activated_grad = dot_nt(cotangent, reduce_weight)
    _, gelu_pull = jax.vjp(exact_gelu, hidden)
    hidden_grad = gelu_pull(activated_grad)[0].astype(BF16)
    expand_bias_grad = column_sum(hidden_grad)
    expand_weight_grad = dot_tn(gathered, hidden_grad).astype(BF16)
    normed_two_grad = scatter(dot_nt(hidden_grad, expand_weight).astype(BF16)).astype(F32)
    own_upstream = lax.dynamic_slice_in_dim(upstream, first_row, share, 0)
    _, second_pull = jax.vjp(layer_norm, middle, feedforward_gain, feedforward_shift)
    middle_grad, second_gain_part, second_shift_part = second_pull(normed_two_grad)
    middle_grad = middle_grad + own_upstream
    branch_grad = gather(middle_grad.astype(BF16))
    output_bias_grad = column_sum(branch_grad)
    output_weight_grad = dot_tn(attended, branch_grad).astype(BF16)
    attended_grad = dot_nt(branch_grad, output_weight).astype(BF16)
    joint_grad = attend_back(queries, keys, values, attended_grad, attended, inverse, weights)
    query_bias_grad = column_sum(joint_grad[0])
    value_bias_grad = column_sum(joint_grad[2])
    input_weight_grad = tuple(dot_tn(normed, part).astype(BF16) for part in joint_grad)
    normed_grad = sum(dot_nt(part, stacked_weight[i]) for i, part in enumerate(joint_grad))
    normed_grad = scatter(normed_grad.astype(BF16)).astype(F32)
    _, first_pull = jax.vjp(layer_norm, own_inputs, attention_gain, attention_shift)
    inputs_grad, first_gain_part, first_shift_part = first_pull(normed_grad)
    tokens_gradient = gather((inputs_grad + middle_grad).astype(BF16))

    norm_parts = lax.psum(
        jnp.stack([first_gain_part, first_shift_part, second_gain_part, second_shift_part]), "tensor"
    )
    small = [
        norm_parts.reshape(-1),
        reduce_bias_grad,
        output_bias_grad,
        query_bias_grad,
        value_bias_grad,
        expand_bias_grad,
    ]
    sizes = [part.shape[0] for part in small]
    sums = lax.psum(
        (
            *input_weight_grad,
            output_weight_grad,
            expand_weight_grad,
            reduce_weight_grad,
            jnp.concatenate(small).astype(BF16),
        ),
        "dp",
    )
    sums = [part.astype(F32) for part in sums]
    ends = [sum(sizes[: i + 1]) for i in range(len(sizes))]
    parts = [sums[6][end - size : end] for size, end in zip(sizes, ends)]
    norms = parts[0].reshape(4, -1)
    return (
        block_out,
        tokens_gradient,
        norms[0],
        norms[1],
        jnp.transpose(jnp.stack(sums[:3]), (1, 0, 2)),
        parts[3],
        parts[4],
        sums[3],
        parts[2],
        norms[2],
        norms[3],
        sums[4],
        parts[5],
        sums[5],
        parts[1],
    )


def solution(mesh):
    in_specs = (
        P("dp", None),
        P(),
        P(),
        P(None, None, "tensor"),
        P("tensor"),
        P("tensor"),
        P("tensor", None),
        P(),
        P(),
        P(),
        P(None, "tensor"),
        P("tensor"),
        P("tensor", None),
        P(),
        P("dp", None),
    )
    out_specs = (
        P("dp", None),
        P("dp", None),
        P(),
        P(),
        P(None, None, "tensor"),
        P("tensor"),
        P("tensor"),
        P("tensor", None),
        P(),
        P(),
        P(),
        P(None, "tensor"),
        P("tensor"),
        P("tensor", None),
        P(),
    )
    return jax.shard_map(shards, mesh=mesh, in_specs=in_specs, out_specs=out_specs, check_vma=False)
```

```python
import functools

import jax
import jax.numpy as jnp
from jax import lax
from jax.experimental import pallas as pl
from jax.experimental.pallas import tpu as pltpu
from jax.sharding import PartitionSpec as P

HEAD_DIM = 64
SEQ = 1568
PAIR = 2 * HEAD_DIM
F32 = jnp.float32
BF16 = jnp.bfloat16
EXP_SCALE = 0.125 * 1.4426950408889634

norm_eps = 1e-06


def layer_norm(values, gain, shift):
    center = values - jnp.mean(values, axis=-1, keepdims=True)
    spread = jnp.mean(center * center, axis=-1, keepdims=True)
    return center * lax.rsqrt(spread + norm_eps) * gain + shift


def exact_gelu(values):
    return jax.nn.gelu(values, approximate=False)


def dot_nn(a, b):
    return lax.dot_general(a, b, (((1,), (0,)), ((), ())), preferred_element_type=F32)


def dot_nt(a, b):
    return lax.dot_general(a, b, (((1,), (1,)), ((), ())), preferred_element_type=F32)


def dot_tn(a, b):
    return lax.dot_general(a, b, (((0,), (0,)), ((), ())), preferred_element_type=F32)


def attend_kernel(q_ref, k_ref, v_ref, out_ref, exact_ref, inverse_ref, weights_ref):
    low_half = lax.broadcasted_iota(jnp.int32, (1, PAIR), 1) < HEAD_DIM
    zero = jnp.zeros((), BF16)
    keys, values, queries = k_ref[...], v_ref[...], q_ref[...]
    mixed, inverses = [], []
    for head in range(2):
        own_keys = jnp.where(low_half if head == 0 else ~low_half, keys, zero)
        scores = dot_nt(queries, own_keys)
        top = jnp.max(scores, axis=1, keepdims=True)
        weights = jnp.exp2((scores - top) * EXP_SCALE)
        inverse = 1.0 / jnp.sum(weights, axis=1, keepdims=True)
        weights = weights.astype(BF16)
        weights_ref[head] = weights
        mixed.append(dot_nn(weights, values) * inverse)
        inverses.append(inverse)
    exact = jnp.where(low_half, mixed[0], mixed[1])
    out_ref[...] = exact.astype(BF16)
    exact_ref[...] = exact
    inverse_ref[...] = jnp.where(low_half, inverses[0], inverses[1])


def attend(queries, keys, values, block=224):
    rows, width = queries.shape
    pairs = width // PAIR
    tile = pl.BlockSpec((block, PAIR), lambda p, i: (i, p))
    whole = pl.BlockSpec((rows, PAIR), lambda p, i: (0, p))
    return pl.pallas_call(
        attend_kernel,
        grid=(pairs, rows // block),
        in_specs=[tile, whole, whole],
        out_specs=[tile, tile, tile, pl.BlockSpec((2, block, rows), lambda p, i: (p, i, 0))],
        out_shape=[
            jax.ShapeDtypeStruct((rows, width), BF16),
            jax.ShapeDtypeStruct((rows, width), F32),
            jax.ShapeDtypeStruct((rows, width), F32),
            jax.ShapeDtypeStruct((2 * pairs, rows, rows), BF16),
        ],
        compiler_params=pltpu.CompilerParams(vmem_limit_bytes=60 << 20),
        cost_estimate=pl.CostEstimate(
            flops=8 * pairs * rows * rows * HEAD_DIM * 4,
            bytes_accessed=4 * pairs * rows * rows,
            transcendentals=2 * pairs * rows * rows,
        ),
        name="attend",
    )(queries, keys, values)


def orders_of(bits):
    if bits == 4:
        return ((0, 1, 2, 3), (1, 0, 2, 3), (2, 0, 1, 3), (2, 1, 0, 3))
    return tuple(tuple((i + j) % bits for j in range(bits)) for i in (0, 1, 2, 3))


class Part:
    def __init__(self, array, first, each, cols, dtype, order):
        self.array, self.first, self.each = array, first, each
        self.cols, self.dtype, self.order = cols, dtype, order


def parts_of(array, shape, dtype, n, shares, orders):
    unit = 16 if dtype == BF16 else 8
    units = shape[0] // (n * unit)
    counts = [units * share // sum(shares) for share in shares]
    counts[0] += units - sum(counts)
    parts, first = [], 0
    for count, order in zip(counts, orders):
        if count:
            parts.append(Part(array, first, count * unit, shape[1], dtype, order))
            first += n * count * unit
    return parts


def divides(shape, dtype, n):
    return shape[0] % (n * (16 if dtype == BF16 else 8)) == 0


class Reduction:
    def __init__(self, parts, n, bufs, lands, gathers, sems):
        self.parts, self.n, self.bits = parts, n, n.bit_length() - 1
        self.bufs, self.lands, self.gathers = bufs, lands, gathers
        self.load_sem, self.store_sem, self.send_sem, self.recv_sem = sems
        me = lax.axis_index("dp")
        self.digit = [(me // (1 << b)) % 2 for b in range(self.bits)]
        self.partner = [me + (1 << b) * (1 - 2 * self.digit[b]) for b in range(self.bits)]

    def greet(self):
        barrier = pltpu.get_barrier_semaphore()
        for b in range(self.bits):
            pl.semaphore_signal(
                barrier, inc=1, device_id={"dp": self.partner[b]}, device_id_type=pl.DeviceIdType.MESH
            )
        pl.semaphore_wait(barrier, self.bits)

    def rows(self, i, position):
        part, shard = self.parts[i], 0
        for level, b in enumerate(part.order):
            flip = (position >> (self.bits - 1 - level)) & 1
            shard = shard + (1 << b) * ((1 - self.digit[b]) if flip else self.digit[b])
        return pl.ds(pl.multiple_of(part.first + shard * part.each, 8), part.each)

    def load(self, i, ref):
        for position in range(self.n):
            pltpu.make_async_copy(ref.at[self.rows(i, position), :], self.bufs[i].at[position], self.load_sem.at[i]).start()

    def load_wait(self, i):
        pltpu.make_async_copy(self.bufs[i], self.bufs[i], self.load_sem.at[i]).wait()

    def store(self, i, ref):
        for position in range(self.n):
            pltpu.make_async_copy(self.gathers[i].at[position], ref.at[self.rows(i, position), :], self.store_sem.at[i]).start()

    def store_wait(self, i):
        pltpu.make_async_copy(self.gathers[i], self.gathers[i], self.store_sem.at[i]).wait()

    def load_own(self, i, ref):
        pltpu.make_async_copy(ref, self.gathers[i].at[0], self.load_sem.at[i]).start()

    def load_own_wait(self, i):
        pltpu.make_async_copy(self.gathers[i].at[0], self.gathers[i].at[0], self.load_sem.at[i]).wait()

    def store_own(self, i, ref):
        pltpu.make_async_copy(self.gathers[i].at[0], ref, self.store_sem.at[i]).start()

    def store_own_wait(self, i):
        pltpu.make_async_copy(self.gathers[i].at[0], self.gathers[i].at[0], self.store_sem.at[i]).wait()

    def exchange(self, i, number):
        level = number if number < self.bits else 2 * self.bits - 1 - number
        half = self.n >> (level + 1)
        if number < self.bits:
            source, target = self.bufs[i].at[pl.ds(half, half)], self.lands[i].at[pl.ds(self.n - 2 * half, half)]
        else:
            source, target = self.gathers[i].at[pl.ds(0, half)], self.gathers[i].at[pl.ds(half, half)]
        k = i * 2 * self.bits + number
        return pltpu.make_async_remote_copy(
            source,
            target,
            self.send_sem.at[k],
            self.recv_sem.at[k],
            device_id={"dp": self.partner[self.parts[i].order[level]]},
            device_id_type=pl.DeviceIdType.MESH,
        )

    def finish(self, i, number):
        self.exchange(i, number).wait()
        if number < self.bits:
            half = self.n >> (number + 1)
            start = self.n - 2 * half
            buf, land = self.bufs[i], self.lands[i]
            to = self.gathers[i] if number == self.bits - 1 else buf

            def add(j, carry):
                to[j] = (buf[j].astype(F32) + land[start + j].astype(F32)).astype(buf.dtype)
                return carry

            lax.fori_loop(0, half, add, 0)


def buffers(summed, gathered, n):
    parts, bits, count = gathered, n.bit_length() - 1, len(gathered)
    return (
        [pltpu.VMEM((n, p.each, p.cols), p.dtype) for p in summed]
        + [pltpu.VMEM((n - 1, p.each, p.cols), p.dtype) for p in summed]
        + [pltpu.VMEM((n, p.each, p.cols), p.dtype) for p in gathered]
        + [pltpu.SemaphoreType.DMA((count,))] * 2
        + [pltpu.SemaphoreType.DMA((count * 2 * bits,))] * 2
    )


def attend_back_kernel(parts, n, arrays, total, *refs):
    q_ref, k_ref, v_ref, g_ref, o_ref, inverse_ref, weights_ref = refs[:7]
    sources, refs = refs[7 : 7 + arrays], refs[7 + arrays :]
    dq_ref, dk_ref, dv_ref = refs[:3]
    owns, refs = refs[3 : 3 + len(parts)], refs[3 + len(parts) :]
    dk_sum, dv_sum = refs[:2]
    refs = refs[2:]
    count = len(parts)
    sums = Reduction(parts, n, refs[:count], refs[count : 2 * count], refs[:count], refs[2 * count :])
    step, steps = pl.program_id(1), pl.num_programs(1)
    low_half = lax.broadcasted_iota(jnp.int32, (1, PAIR), 1) < HEAD_DIM
    zero = jnp.zeros((), BF16)
    now = pl.program_id(0) * steps + step

    @pl.when(now == 0)
    def _():
        sums.greet()
        for i in range(count):
            sums.load(i, sources[parts[i].array])
        for i in range(count):
            sums.load_wait(i)
            sums.exchange(i, 0).start()

    def advance(i, number):
        sums.finish(i, number)
        if number + 1 < sums.bits:
            sums.exchange(i, number + 1).start()
        else:
            sums.store_own(i, owns[i])

    events = [(i, number) for number in range(sums.bits) for i in range(count)]
    slots = []
    for i, number in events:
        first, last = EVENT_TIMES[min(number, 3)]
        slots.append(min(total, int((first + (last - first) * i / max(count - 1, 1)) * total)))
    for slot in sorted(set(slots)):
        if slot < total:

            @pl.when(now == slot)
            def _(slot=slot):
                for event, place in zip(events, slots):
                    if place == slot:
                        advance(*event)

    @pl.when(step == 0)
    def _():
        dk_sum[...] = jnp.zeros_like(dk_sum)
        dv_sum[...] = jnp.zeros_like(dv_sum)

    keys, values, queries = k_ref[...], v_ref[...], q_ref[...]
    grads = (g_ref[...].astype(F32) * inverse_ref[...]).astype(BF16)
    products = grads.astype(F32) * o_ref[...]
    query_grad = None
    for head in range(2):
        own = low_half if head == 0 else ~low_half
        inner = jnp.sum(jnp.where(own, products, 0.0), axis=1, keepdims=True)
        weights = weights_ref[head]
        pushed = dot_nt(grads, jnp.where(own, values, zero))
        score_grad = (weights.astype(F32) * (pushed - inner)).astype(BF16)
        part = dot_nn(score_grad, jnp.where(own, keys, zero))
        query_grad = part if query_grad is None else query_grad + part
        dv_sum[...] += dot_tn(weights, jnp.where(own, grads, zero))
        dk_sum[...] += dot_tn(score_grad, jnp.where(own, queries, zero))
    dq_ref[...] = (query_grad * 0.125).astype(BF16)

    @pl.when(step == steps - 1)
    def _():
        dk_ref[...] = (dk_sum[...] * 0.125).astype(BF16)
        dv_ref[...] = dv_sum[...].astype(BF16)

    @pl.when(now == total - 1)
    def _():
        for event, place in zip(events, slots):
            if place == total:
                advance(*event)
        for i in range(count):
            sums.store_own_wait(i)


def attend_back(queries, keys, values, grads, outs, inverse, weights, sources, parts, n, block=224):
    rows, width = queries.shape
    pairs = width // PAIR
    tile = pl.BlockSpec((block, PAIR), lambda p, i: (i, p))
    whole = pl.BlockSpec((rows, PAIR), lambda p, i: (0, p))
    anywhere = pl.BlockSpec(memory_space=pl.ANY)
    results = pl.pallas_call(
        functools.partial(attend_back_kernel, parts, n, len(sources), pairs * (rows // block)),
        grid=(pairs, rows // block),
        in_specs=[tile, whole, whole, tile, tile, tile, pl.BlockSpec((2, block, rows), lambda p, i: (p, i, 0))]
        + [anywhere] * len(sources),
        out_specs=[tile, whole, whole] + [anywhere] * len(parts),
        out_shape=[jax.ShapeDtypeStruct((rows, width), BF16)] * 3
        + [jax.ShapeDtypeStruct((p.each, p.cols), p.dtype) for p in parts],
        scratch_shapes=[pltpu.VMEM((rows, PAIR), F32)] * 2 + buffers(parts, [], n)[: 2 * len(parts)] + buffers([], parts, n)[len(parts) :],
        compiler_params=pltpu.CompilerParams(vmem_limit_bytes=60 << 20, collective_id=0, has_side_effects=True),
        cost_estimate=pl.CostEstimate(
            flops=16 * pairs * rows * rows * HEAD_DIM * 4,
            bytes_accessed=4 * pairs * rows * rows,
            transcendentals=0,
        ),
        name="attend_back",
    )(queries, keys, values, grads, outs, inverse, weights, *sources)
    return results[:3], results[3:]


def spread_kernel(own_parts, full_parts, n, own_arrays, full_arrays, *refs):
    owns, refs = refs[: len(own_parts)], refs[len(own_parts) :]
    sources, refs = refs[:full_arrays], refs[full_arrays:]
    spread, refs = refs[:own_arrays], refs[own_arrays:]
    summed, refs = refs[:full_arrays], refs[full_arrays:]
    parts = own_parts + full_parts
    count, skip = len(parts), len(own_parts)
    full = len(full_parts)
    bufs, lands, gathers = refs[:full], refs[full : 2 * full], refs[2 * full : 2 * full + count]
    none = (None,) * skip
    sums = Reduction(parts, n, none + bufs, none + lands, gathers, refs[2 * full + count :])
    last = 2 * sums.bits
    sums.greet()
    for i in range(skip):
        sums.load_own(i, owns[i])
    for i in range(skip, count):
        sums.load(i, sources[parts[i].array])

    def step(i, number):
        if i < skip and number == sums.bits:
            sums.load_own_wait(i)
        elif number == 0:
            sums.load_wait(i)
        else:
            sums.finish(i, number - 1)
        if number < last:
            sums.exchange(i, number).start()
        else:
            sums.store(i, (spread if i < skip else summed)[parts[i].array])

    for turn in range(last + 2):
        if turn <= last:
            for i in range(skip, count):
                step(i, turn)
        number = turn - 1
        if sums.bits <= number <= last:
            for i in range(skip):
                step(i, number)
    for i in range(count):
        sums.store_wait(i)


def spread_and_sum(owns, own_parts, own_shapes, sources, full_parts, n):
    anywhere = pl.BlockSpec(memory_space=pl.ANY)
    shapes = list(own_shapes) + [jax.ShapeDtypeStruct(s.shape, s.dtype) for s in sources]
    results = pl.pallas_call(
        functools.partial(spread_kernel, own_parts, full_parts, n, len(own_shapes), len(sources)),
        in_specs=[anywhere] * (len(owns) + len(sources)),
        out_specs=[anywhere] * len(shapes),
        out_shape=shapes,
        scratch_shapes=buffers(full_parts, own_parts + full_parts, n),
        compiler_params=pltpu.CompilerParams(vmem_limit_bytes=60 << 20, collective_id=1, has_side_effects=True),
        name="spread_and_sum",
    )(*owns, *sources)
    return results[: len(own_shapes)], results[len(own_shapes) :]


EVENT_TIMES = ((0.3, 0.58), (0.62, 0.88), (0.9, 1.0), (1.0, 1.0))


def column_sum(values):
    return jnp.sum(values, axis=0, dtype=F32)


def shards(
    tokens,
    attention_gain,
    attention_shift,
    input_weight,
    query_bias,
    value_bias,
    output_weight,
    output_bias,
    feedforward_gain,
    feedforward_shift,
    expand_weight,
    expand_bias,
    reduce_weight,
    reduce_bias,
    cotangent,
):
    rows = tokens.shape[0]
    share = rows // lax.axis_size("tensor")
    first_row = lax.axis_index("tensor") * share

    def scatter(values):
        return lax.psum_scatter(values, "tensor", scatter_dimension=0, tiled=True)

    def gather(values):
        return lax.all_gather(values, "tensor", axis=0, tiled=True)

    stacked_weight = jnp.transpose(input_weight, (1, 0, 2))
    inputs = tokens.astype(F32)
    upstream = cotangent.astype(F32)
    normed = layer_norm(inputs, attention_gain, attention_shift).astype(BF16)
    queries = (dot_nn(normed, stacked_weight[0]) + query_bias).astype(BF16)
    keys = dot_nn(normed, stacked_weight[1]).astype(BF16)
    values = (dot_nn(normed, stacked_weight[2]) + value_bias).astype(BF16)
    attended, exact, inverse, weights = attend(queries, keys, values)
    own_inputs = lax.dynamic_slice_in_dim(inputs, first_row, share, 0)
    middle = own_inputs + scatter(dot_nn(attended, output_weight).astype(BF16)).astype(F32) + output_bias
    normed_two = layer_norm(middle, feedforward_gain, feedforward_shift).astype(BF16)
    gathered = gather(normed_two)
    hidden = dot_nn(gathered, expand_weight) + expand_bias
    activated = exact_gelu(hidden).astype(BF16)
    result = middle + (scatter(dot_nn(activated, reduce_weight).astype(BF16)).astype(F32) + reduce_bias)
    block_out = gather(result.astype(BF16))
    reduce_bias_grad = column_sum(upstream)
    reduce_weight_grad = dot_tn(activated, cotangent).astype(BF16)
    activated_grad = dot_nt(cotangent, reduce_weight)
    _, gelu_pull = jax.vjp(exact_gelu, hidden)
    hidden_grad = gelu_pull(activated_grad)[0].astype(BF16)
    expand_bias_grad = column_sum(hidden_grad)
    expand_weight_grad = dot_tn(gathered, hidden_grad).astype(BF16)
    normed_two_grad = scatter(dot_nt(hidden_grad, expand_weight).astype(BF16)).astype(F32)
    own_upstream = lax.dynamic_slice_in_dim(upstream, first_row, share, 0)
    _, second_pull = jax.vjp(layer_norm, middle, feedforward_gain, feedforward_shift)
    middle_grad, second_gain_part, second_shift_part = second_pull(normed_two_grad)
    middle_grad = middle_grad + own_upstream
    branch_grad = gather(middle_grad.astype(BF16))
    output_bias_grad = column_sum(branch_grad)
    output_weight_grad = dot_tn(attended, branch_grad).astype(BF16)
    attended_grad = dot_nt(branch_grad, output_weight).astype(BF16)
    n = lax.axis_size("dp")
    orders = orders_of(n.bit_length() - 1)
    feed = (reduce_weight_grad, expand_weight_grad)
    feed_parts = parts_of(0, feed[0].shape, BF16, n, (3, 3, 2), orders[:3]) + parts_of(
        1, feed[1].shape, BF16, n, (1, 1, 2), (orders[0], orders[1], orders[3])
    )
    joint_grad, owns = attend_back(
        queries, keys, values, attended_grad, exact, inverse, weights, feed, feed_parts, n
    )
    query_bias_grad = column_sum(joint_grad[0])
    value_bias_grad = column_sum(joint_grad[2])
    input_weight_grad = tuple(dot_tn(normed, part).astype(BF16) for part in joint_grad)
    normed_grad = sum(dot_nt(part, stacked_weight[i]) for i, part in enumerate(joint_grad))
    normed_grad = scatter(normed_grad.astype(BF16)).astype(F32)
    _, first_pull = jax.vjp(layer_norm, own_inputs, attention_gain, attention_shift)
    inputs_grad, first_gain_part, first_shift_part = first_pull(normed_grad)
    tokens_gradient = gather((inputs_grad + middle_grad).astype(BF16))

    norm_parts = lax.psum(
        jnp.stack([first_gain_part, first_shift_part, second_gain_part, second_shift_part]), "tensor"
    )
    small = [
        norm_parts.reshape(-1),
        reduce_bias_grad,
        output_bias_grad,
        query_bias_grad,
        value_bias_grad,
        expand_bias_grad,
    ]
    sizes = [part.shape[0] for part in small]
    table_rows = -(-sum(sizes) // (n * 8 * 128)) * n * 8
    table = jnp.pad(jnp.concatenate(small), (0, table_rows * 128 - sum(sizes))).reshape(table_rows, 128)
    rest = [*input_weight_grad, output_weight_grad, table]
    fits = [divides(part.shape, part.dtype, n) for part in rest]
    sources, rest_parts = [], []
    for which, part in enumerate(rest):
        if fits[which]:
            rest_parts += parts_of(len(sources), part.shape, part.dtype, n, (1,), (orders[which % 4],))
            sources.append(part)
    shapes = [jax.ShapeDtypeStruct(part.shape, part.dtype) for part in feed]
    feed, summed = spread_and_sum(owns, feed_parts, shapes, sources, rest_parts, n)
    summed = list(summed)
    rest = [summed.pop(0) if fit else lax.psum(part, "dp") for part, fit in zip(rest, fits)]
    sums = [part.astype(F32) for part in (*rest[:4], feed[1], feed[0])]
    flat = rest[4].reshape(-1)
    ends = [sum(sizes[: i + 1]) for i in range(len(sizes))]
    parts = [flat[end - size : end] for size, end in zip(sizes, ends)]
    norms = parts[0].reshape(4, -1)
    return (
        block_out,
        tokens_gradient,
        norms[0],
        norms[1],
        jnp.transpose(jnp.stack(sums[:3]), (1, 0, 2)),
        parts[3],
        parts[4],
        sums[3],
        parts[2],
        norms[2],
        norms[3],
        sums[4],
        parts[5],
        sums[5],
        parts[1],
    )


def solution(mesh):
    in_specs = (
        P("dp", None),
        P(),
        P(),
        P(None, None, "tensor"),
        P("tensor"),
        P("tensor"),
        P("tensor", None),
        P(),
        P(),
        P(),
        P(None, "tensor"),
        P("tensor"),
        P("tensor", None),
        P(),
        P("dp", None),
    )
    out_specs = (
        P("dp", None),
        P("dp", None),
        P(),
        P(),
        P(None, None, "tensor"),
        P("tensor"),
        P("tensor"),
        P("tensor", None),
        P(),
        P(),
        P(),
        P(None, "tensor"),
        P("tensor"),
        P("tensor", None),
        P(),
    )
    return jax.shard_map(shards, mesh=mesh, in_specs=in_specs, out_specs=out_specs, check_vma=False)
```

```python
import functools

import jax
import jax.numpy as jnp
from jax import lax
from jax.experimental import pallas as pl
from jax.experimental.pallas import tpu as pltpu
from jax.sharding import PartitionSpec as P

HEAD_DIM = 64
SEQ = 1568
PAIR = 2 * HEAD_DIM
F32 = jnp.float32
BF16 = jnp.bfloat16
EXP_SCALE = 0.125 * 1.4426950408889634

norm_eps = 1e-06


def layer_norm(values, gain, shift):
    center = values - jnp.mean(values, axis=-1, keepdims=True)
    spread = jnp.mean(center * center, axis=-1, keepdims=True)
    return center * lax.rsqrt(spread + norm_eps) * gain + shift


def dot_nn(a, b):
    return lax.dot_general(a, b, (((1,), (0,)), ((), ())), preferred_element_type=F32)


def dot_nt(a, b):
    return lax.dot_general(a, b, (((1,), (1,)), ((), ())), preferred_element_type=F32)


def dot_tn(a, b):
    return lax.dot_general(a, b, (((0,), (0,)), ((), ())), preferred_element_type=F32)


def attend_kernel(q_ref, k_ref, v_ref, out_ref, exact_ref, inverse_ref, weights_ref):
    low_half = lax.broadcasted_iota(jnp.int32, (1, PAIR), 1) < HEAD_DIM
    zero = jnp.zeros((), BF16)
    keys, values, queries = k_ref[...], v_ref[...], q_ref[...]
    mixed, inverses = [], []
    for head in range(2):
        own_keys = jnp.where(low_half if head == 0 else ~low_half, keys, zero)
        scores = dot_nt(queries, own_keys)
        top = jnp.max(scores, axis=1, keepdims=True)
        weights = jnp.exp2((scores - top) * EXP_SCALE)
        inverse = 1.0 / jnp.sum(weights, axis=1, keepdims=True)
        weights = weights.astype(BF16)
        weights_ref[head] = weights
        mixed.append(dot_nn(weights, values) * inverse)
        inverses.append(inverse)
    exact = jnp.where(low_half, mixed[0], mixed[1])
    out_ref[...] = exact.astype(BF16)
    exact_ref[...] = exact
    inverse_ref[...] = jnp.where(low_half, inverses[0], inverses[1])


def attend(queries, keys, values, block=224):
    rows, width = queries.shape
    pairs = width // PAIR
    tile = pl.BlockSpec((block, PAIR), lambda p, i: (i, p))
    whole = pl.BlockSpec((rows, PAIR), lambda p, i: (0, p))
    return pl.pallas_call(
        attend_kernel,
        grid=(pairs, rows // block),
        in_specs=[tile, whole, whole],
        out_specs=[tile, tile, tile, pl.BlockSpec((2, block, rows), lambda p, i: (p, i, 0))],
        out_shape=[
            jax.ShapeDtypeStruct((rows, width), BF16),
            jax.ShapeDtypeStruct((rows, width), F32),
            jax.ShapeDtypeStruct((rows, width), F32),
            jax.ShapeDtypeStruct((2 * pairs, rows, rows), BF16),
        ],
        compiler_params=pltpu.CompilerParams(vmem_limit_bytes=60 << 20),
        cost_estimate=pl.CostEstimate(
            flops=8 * pairs * rows * rows * HEAD_DIM * 4,
            bytes_accessed=4 * pairs * rows * rows,
            transcendentals=2 * pairs * rows * rows,
        ),
        name="attend",
    )(queries, keys, values)


def feed_kernel(n_ref, c_ref, expand_ref, reduce_ref, bias_ref, act_ref, grad_ref, sum_ref, *, chunk):
    @pl.when(pl.program_id(0) == 0)
    def _():
        sum_ref[...] = jnp.zeros_like(sum_ref)

    normed, cotangent = n_ref[...], c_ref[...]
    for first in range(0, expand_ref.shape[1], chunk):
        cols = pl.ds(first, chunk)
        hidden = dot_nn(normed, expand_ref[:, cols]) + bias_ref[:, cols]
        pushed = dot_nt(cotangent, reduce_ref[cols, :])
        share = 0.5 * lax.erf(hidden * ROOT_HALF) + 0.5
        act_ref[:, cols] = (hidden * share).astype(BF16)
        density = jnp.exp2(hidden * hidden * HALF_LOG2E) * NORMAL_PEAK
        grad = (pushed * (share + hidden * density)).astype(BF16)
        grad_ref[:, cols] = grad
        sum_ref[:, cols] += jnp.sum(grad.astype(F32), axis=0, keepdims=True)


def feed(normed, cotangent, expand_weight, reduce_weight, expand_bias, block=224, chunk=256):
    rows, depth = normed.shape
    width = expand_weight.shape[1]
    tile = pl.BlockSpec((block, depth), lambda i: (i, 0))
    out = pl.BlockSpec((block, width), lambda i: (i, 0))

    def whole(shape):
        return pl.BlockSpec(shape, lambda i: (0, 0))

    act, grad, total = pl.pallas_call(
        functools.partial(feed_kernel, chunk=chunk),
        grid=(rows // block,),
        in_specs=[tile, tile, whole((depth, width)), whole((width, depth)), whole((1, width))],
        out_specs=[out, out, whole((1, width))],
        out_shape=[jax.ShapeDtypeStruct((rows, width), BF16)] * 2 + [jax.ShapeDtypeStruct((1, width), F32)],
        compiler_params=pltpu.CompilerParams(vmem_limit_bytes=60 << 20),
        cost_estimate=pl.CostEstimate(
            flops=4 * rows * depth * width, bytes_accessed=8 * rows * (depth + width), transcendentals=rows * width
        ),
        name="feed",
    )(normed, cotangent, expand_weight, reduce_weight, expand_bias.reshape(1, -1))
    return act, grad, total.reshape(-1)


def orders_of(bits):
    if bits == 4:
        return ((0, 1, 2, 3), (1, 0, 2, 3), (2, 0, 1, 3), (2, 1, 0, 3))
    return tuple(tuple((i + j) % bits for j in range(bits)) for i in (0, 1, 2, 3))


class Part:
    def __init__(self, array, first, each, cols, dtype, order, outer):
        self.array, self.first, self.each = array, first, each
        self.cols, self.dtype, self.order, self.outer = cols, dtype, order, outer
        self.inner = order[1:] if outer else order
        self.depth = len(self.inner)
        self.shards = 1 << self.depth
        self.half_rows = self.shards * each


def parts_of(array, shape, dtype, n, shares, orders, outer=True):
    unit = 16 if dtype == BF16 else 8
    units = shape[0] // (n * unit)
    counts = [units * share // sum(shares) for share in shares]
    counts[0] += units - sum(counts)
    parts, first = [], 0
    for count, order in zip(counts, orders):
        if count:
            parts.append(Part(array, first, count * unit, shape[1], dtype, order, outer))
            first += n * count * unit
    return parts


def divides(shape, dtype, n):
    return shape[0] % (n * (16 if dtype == BF16 else 8)) == 0


def swap_bit(values, bit, n):
    return lax.ppermute(values, "dp", [(j, j ^ (1 << bit)) for j in range(n)])


def bit_of_index(bit):
    return (lax.axis_index("dp") >> bit) & 1


def outer_halving(array, part, n):
    other = 1 - bit_of_index(part.order[0])
    half = lax.dynamic_slice_in_dim(array, part.first + other * part.half_rows, part.half_rows, 0)
    return swap_bit(half, part.order[0], n)


def outer_doubling(own, part, n):
    other = swap_bit(own, part.order[0], n)
    low = bit_of_index(part.order[0]) == 0
    return [jnp.where(low, own, other).astype(F32), jnp.where(low, other, own).astype(F32)]


class Reduction:
    def __init__(self, parts, bits, bufs, lands, gathers, sems):
        self.parts, self.bits = parts, bits
        self.bufs, self.lands, self.gathers = bufs, lands, gathers
        self.load_sem, self.store_sem, self.send_sem, self.recv_sem = sems
        me = lax.axis_index("dp")
        self.digit = [(me // (1 << b)) % 2 for b in range(bits)]
        self.partner = [me + (1 << b) * (1 - 2 * self.digit[b]) for b in range(bits)]

    def greet(self):
        barrier = pltpu.get_barrier_semaphore()
        for b in range(self.bits):
            pl.semaphore_signal(
                barrier, inc=1, device_id={"dp": self.partner[b]}, device_id_type=pl.DeviceIdType.MESH
            )
        pl.semaphore_wait(barrier, self.bits)

    def rows(self, i, position, base=0):
        part, shard = self.parts[i], 0
        for level, b in enumerate(part.inner):
            flip = (position >> (part.depth - 1 - level)) & 1
            shard = shard + (1 << (part.depth - 1 - level)) * ((1 - self.digit[b]) if flip else self.digit[b])
        return pl.ds(pl.multiple_of(base + shard * part.each, 8), part.each)

    def load(self, i, ref, recv):
        part = self.parts[i]
        base = part.first + (self.digit[part.order[0]] * part.half_rows if part.outer else 0)
        for position in range(part.shards):
            pltpu.make_async_copy(
                ref.at[self.rows(i, position, base), :], self.bufs[i].at[position], self.load_sem.at[2 * i]
            ).start()
            if part.outer:
                pltpu.make_async_copy(
                    recv.at[self.rows(i, position), :], self.lands[i].at[position], self.load_sem.at[2 * i + 1]
                ).start()

    def load_own(self, i, ref):
        pltpu.make_async_copy(ref, self.gathers[i].at[0], self.load_sem.at[2 * i]).start()

    def begin(self, i):
        part, buf, land = self.parts[i], self.bufs[i], self.lands[i]
        pltpu.make_async_copy(buf, buf, self.load_sem.at[2 * i]).wait()
        if part.outer:
            got = land.at[pl.ds(0, part.shards)]
            pltpu.make_async_copy(got, got, self.load_sem.at[2 * i + 1]).wait()
            self.add(i, 0, part.shards, buf)

    def begin_own(self, i):
        own = self.gathers[i].at[0]
        pltpu.make_async_copy(own, own, self.load_sem.at[2 * i]).wait()

    def add(self, i, start, count, to):
        buf, land = self.bufs[i], self.lands[i]

        def body(j, carry):
            to[j] = (buf[j].astype(F32) + land[start + j].astype(F32)).astype(buf.dtype)
            return carry

        lax.fori_loop(0, count, body, 0)

    def store(self, i, ref):
        base = 0 if self.parts[i].outer else self.parts[i].first
        for position in range(self.parts[i].shards):
            pltpu.make_async_copy(
                self.gathers[i].at[position], ref.at[self.rows(i, position, base), :], self.store_sem.at[i]
            ).start()

    def store_wait(self, i):
        pltpu.make_async_copy(self.gathers[i], self.gathers[i], self.store_sem.at[i]).wait()

    def store_own(self, i, ref):
        pltpu.make_async_copy(self.gathers[i].at[0], ref, self.store_sem.at[i]).start()

    def store_own_wait(self, i):
        own = self.gathers[i].at[0]
        pltpu.make_async_copy(own, own, self.store_sem.at[i]).wait()

    def exchange(self, i, number):
        part = self.parts[i]
        level = number if number < part.depth else 2 * part.depth - 1 - number
        half = part.shards >> (level + 1)
        if number < part.depth:
            at = (part.shards if part.outer else 0) + part.shards - 2 * half
            source, target = self.bufs[i].at[pl.ds(half, half)], self.lands[i].at[pl.ds(at, half)]
        else:
            source, target = self.gathers[i].at[pl.ds(0, half)], self.gathers[i].at[pl.ds(half, half)]
        k = sum(2 * p.depth for p in self.parts[:i]) + number
        return pltpu.make_async_remote_copy(
            source,
            target,
            self.send_sem.at[k],
            self.recv_sem.at[k],
            device_id={"dp": self.partner[part.inner[level]]},
            device_id_type=pl.DeviceIdType.MESH,
        )

    def finish(self, i, number):
        self.exchange(i, number).wait()
        part = self.parts[i]
        if number < part.depth:
            half = part.shards >> (number + 1)
            at = (part.shards if part.outer else 0) + part.shards - 2 * half
            self.add(i, at, half, self.gathers[i] if number == part.depth - 1 else self.bufs[i])


def buffers(summed, gathered):
    return (
        [pltpu.VMEM((p.shards, p.each, p.cols), p.dtype) for p in summed]
        + [pltpu.VMEM((p.shards * (2 if p.outer else 1) - 1, p.each, p.cols), p.dtype) for p in summed]
        + [pltpu.VMEM((p.shards, p.each, p.cols), p.dtype) for p in gathered]
    )


def semaphores(parts):
    exchanges = sum(2 * p.depth for p in parts)
    return [
        pltpu.SemaphoreType.DMA((2 * len(parts),)),
        pltpu.SemaphoreType.DMA((len(parts),)),
        pltpu.SemaphoreType.DMA((exchanges,)),
        pltpu.SemaphoreType.DMA((exchanges,)),
    ]


def attend_back_kernel(parts, early, bits, arrays, total, *refs):
    count = len(parts)
    q_ref, k_ref, v_ref, g_ref, o_ref, inverse_ref, weights_ref = refs[:7]
    sources, recvs, refs = refs[7 : 7 + arrays], refs[7 + arrays : 7 + arrays + count], refs[7 + arrays + count :]
    dq_ref, dk_ref, dv_ref = refs[:3]
    results, refs = refs[3 : 3 + count], refs[3 + count :]
    dk_sum, dv_sum = refs[:2]
    refs = refs[2:]
    sums = Reduction(
        parts, bits, refs[:count], refs[count : 2 * count], refs[2 * count : 3 * count], refs[3 * count :]
    )
    step, steps = pl.program_id(1), pl.num_programs(1)
    low_half = lax.broadcasted_iota(jnp.int32, (1, PAIR), 1) < HEAD_DIM
    zero = jnp.zeros((), BF16)
    now = pl.program_id(0) * steps + step

    @pl.when(now == 0)
    def _():
        for i in range(count):
            sums.load(i, sources[parts[i].array], recvs[i])
        sums.greet()
        for i in range(count):
            sums.begin(i)
            sums.exchange(i, 0).start()

    def advance(i, number):
        sums.finish(i, number)
        last = (2 if i < early else 1) * parts[i].depth - 1
        if number < last:
            sums.exchange(i, number + 1).start()
        elif i < early:
            sums.store(i, results[i])
        else:
            sums.store_own(i, results[i])

    depth = bits - 1
    events = [(i, number) for number in range(2 * depth) for i in range(count if number < depth else early)]
    slots = []
    for at, (i, number) in enumerate(events):
        first, last = EVENT_TIMES[min(number, len(EVENT_TIMES) - 1)]
        slots.append(min(total, int((first + (last - first) * i / max(count - 1, 1)) * total)))
    for slot in sorted(set(slots)):
        if slot < total:

            @pl.when(now == slot)
            def _(slot=slot):
                for event, place in zip(events, slots):
                    if place == slot:
                        advance(*event)

    @pl.when(step == 0)
    def _():
        dk_sum[...] = jnp.zeros_like(dk_sum)
        dv_sum[...] = jnp.zeros_like(dv_sum)

    keys, values, queries = k_ref[...], v_ref[...], q_ref[...]
    grads = (g_ref[...].astype(F32) * inverse_ref[...]).astype(BF16)
    products = grads.astype(F32) * o_ref[...]
    query_grad = None
    for head in range(2):
        own = low_half if head == 0 else ~low_half
        inner = jnp.sum(jnp.where(own, products, 0.0), axis=1, keepdims=True)
        weights = weights_ref[head]
        pushed = dot_nt(grads, jnp.where(own, values, zero))
        score_grad = (weights.astype(F32) * (pushed - inner)).astype(BF16)
        part = dot_nn(score_grad, jnp.where(own, keys, zero))
        query_grad = part if query_grad is None else query_grad + part
        dv_sum[...] += dot_tn(weights, jnp.where(own, grads, zero))
        dk_sum[...] += dot_tn(score_grad, jnp.where(own, queries, zero))
    dq_ref[...] = (query_grad * 0.125).astype(BF16)

    @pl.when(step == steps - 1)
    def _():
        dk_ref[...] = (dk_sum[...] * 0.125).astype(BF16)
        dv_ref[...] = dv_sum[...].astype(BF16)

    @pl.when(now == total - 1)
    def _():
        for event, place in zip(events, slots):
            if place == total:
                advance(*event)
        for i in range(count):
            if i < early:
                sums.store_wait(i)
            else:
                sums.store_own_wait(i)


def attend_back(queries, keys, values, grads, outs, inverse, weights, sources, recvs, parts, early, bits, block=224):
    rows, width = queries.shape
    pairs = width // PAIR
    tile = pl.BlockSpec((block, PAIR), lambda p, i: (i, p))
    whole = pl.BlockSpec((rows, PAIR), lambda p, i: (0, p))
    anywhere = pl.BlockSpec(memory_space=pl.ANY)
    results = pl.pallas_call(
        functools.partial(attend_back_kernel, parts, early, bits, len(sources), pairs * (rows // block)),
        grid=(pairs, rows // block),
        in_specs=[tile, whole, whole, tile, tile, tile, pl.BlockSpec((2, block, rows), lambda p, i: (p, i, 0))]
        + [anywhere] * (len(sources) + len(recvs)),
        out_specs=[tile, whole, whole] + [anywhere] * len(parts),
        out_shape=[jax.ShapeDtypeStruct((rows, width), BF16)] * 3
        + [
            jax.ShapeDtypeStruct((p.half_rows if i < early else p.each, p.cols), p.dtype)
            for i, p in enumerate(parts)
        ],
        scratch_shapes=[pltpu.VMEM((rows, PAIR), F32)] * 2 + buffers(parts, parts) + semaphores(parts),
        compiler_params=pltpu.CompilerParams(vmem_limit_bytes=60 << 20, collective_id=0, has_side_effects=True),
        cost_estimate=pl.CostEstimate(
            flops=16 * pairs * rows * rows * HEAD_DIM * 4,
            bytes_accessed=4 * pairs * rows * rows,
            transcendentals=0,
        ),
        name="attend_back",
    )(queries, keys, values, grads, outs, inverse, weights, *sources, *recvs)
    return results[:3], results[3:]


def rest_kernel(own_parts, full_parts, bits, arrays, *refs):
    skip, full = len(own_parts), len(full_parts)
    parts, count = own_parts + full_parts, skip + full
    owns, sources, refs = refs[:skip], refs[skip : skip + arrays], refs[skip + arrays :]
    outer = [i for i, p in enumerate(parts) if i >= skip and p.outer]
    recvs, refs = dict(zip(outer, refs[: len(outer)])), refs[len(outer) :]
    results, refs = refs[:count], refs[count:]
    none = (None,) * skip
    bufs, lands, gathers = refs[:full], refs[full : 2 * full], refs[2 * full : 2 * full + count]
    sums = Reduction(parts, bits, none + bufs, none + lands, gathers, refs[2 * full + count :])
    for i in range(skip):
        sums.load_own(i, owns[i])
    for i in range(skip, count):
        sums.load(i, sources[parts[i].array], recvs.get(i))
    sums.greet()

    def step(i, number):
        depth = parts[i].depth
        if i < skip and number == depth:
            sums.begin_own(i)
        elif number == 0:
            sums.begin(i)
        else:
            sums.finish(i, number - 1)
        if number < 2 * depth:
            sums.exchange(i, number).start()
        else:
            sums.store(i, results[i])

    for turn in range(2 * bits + 1):
        for i in range(skip, count):
            if turn <= 2 * parts[i].depth:
                step(i, turn)
        for i in range(skip):
            number = turn - OWN_DELAY + parts[i].depth
            if parts[i].depth <= number <= 2 * parts[i].depth:
                step(i, number)
    for i in range(count):
        sums.store_wait(i)


def rest_sums(owns, own_parts, sources, recvs, full_parts, bits):
    anywhere = pl.BlockSpec(memory_space=pl.ANY)
    parts = own_parts + full_parts
    shapes = [
        jax.ShapeDtypeStruct((p.half_rows if p.outer else p.first + p.shards * p.each, p.cols), p.dtype)
        for p in parts
    ]
    results = pl.pallas_call(
        functools.partial(rest_kernel, own_parts, full_parts, bits, len(sources)),
        in_specs=[anywhere] * (len(owns) + len(sources) + len(recvs)),
        out_specs=[anywhere] * len(shapes),
        out_shape=shapes,
        scratch_shapes=buffers(full_parts, parts) + semaphores(parts),
        compiler_params=pltpu.CompilerParams(vmem_limit_bytes=60 << 20, collective_id=1, has_side_effects=True),
        name="rest_sums",
    )(*owns, *sources, *recvs)
    return results[: len(owns)], results[len(owns) :]


EVENT_TIMES = ((0.18, 0.45), (0.47, 0.57), (0.6, 0.85), (0.9, 1.0), (1.0, 1.0))
EARLY = 3
OWN_DELAY = 1
ROOT_HALF = 0.7071067811865476
HALF_LOG2E = -0.5 * 1.4426950408889634
NORMAL_PEAK = 0.3989422804014327


def column_sum(values):
    return jnp.sum(values, axis=0, dtype=F32)


def shards(
    tokens,
    attention_gain,
    attention_shift,
    input_weight,
    query_bias,
    value_bias,
    output_weight,
    output_bias,
    feedforward_gain,
    feedforward_shift,
    expand_weight,
    expand_bias,
    reduce_weight,
    reduce_bias,
    cotangent,
):
    rows = tokens.shape[0]
    cores = lax.axis_size("tensor")
    core = lax.axis_index("tensor")
    share = rows // cores
    n = lax.axis_size("dp")
    bits = n.bit_length() - 1
    orders = orders_of(bits)

    if cores == 2:

        def own_first(values):
            own = lax.dynamic_slice_in_dim(values, core * share, share, 0)
            return jnp.concatenate([own, lax.dynamic_slice_in_dim(values, (1 - core) * share, share, 0)])

        def swap(values):
            return lax.ppermute(values, "tensor", [(0, 1), (1, 0)])

        def scatter(product, values):
            other = swap(product(*(v[share:] for v in values)).astype(BF16))
            return product(*(v[:share] for v in values)) + other.astype(F32)

        def gather(values):
            return jnp.concatenate([values, swap(values)])

        def gather_in_order(values):
            other = swap(values)
            first = core == 0
            return jnp.concatenate([jnp.where(first, values, other), jnp.where(first, other, values)])

        first_row = 0
    else:

        def own_first(values):
            return values

        def scatter(product, values):
            return lax.psum_scatter(product(*values).astype(BF16), "tensor", scatter_dimension=0, tiled=True).astype(F32)

        def gather(values):
            return lax.all_gather(values, "tensor", axis=0, tiled=True)

        gather_in_order = gather
        first_row = core * share

    def own_rows(values):
        if cores == 2:
            return values[:share]
        return lax.dynamic_slice_in_dim(values, first_row, share, 0)

    stacked_weight = jnp.transpose(input_weight, (1, 0, 2))
    tokens = own_first(tokens)
    cotangent = own_first(cotangent)
    inputs = tokens.astype(F32)
    normed = layer_norm(inputs, attention_gain, attention_shift).astype(BF16)
    queries = (dot_nn(normed, stacked_weight[0]) + query_bias).astype(BF16)
    keys = dot_nn(normed, stacked_weight[1]).astype(BF16)
    values = (dot_nn(normed, stacked_weight[2]) + value_bias).astype(BF16)
    attended, exact, inverse, weights = attend(queries, keys, values)
    own_inputs = own_rows(tokens).astype(F32)
    middle = own_inputs + scatter(lambda part: dot_nn(part, output_weight), (attended,)) + output_bias
    normed_two = layer_norm(middle, feedforward_gain, feedforward_shift).astype(BF16)
    gathered = gather(normed_two)
    activated, hidden_grad, expand_bias_grad = feed(gathered, cotangent, expand_weight, reduce_weight, expand_bias)
    reduce_weight_grad = dot_tn(activated, cotangent).astype(BF16)
    expand_weight_grad = dot_tn(gathered, hidden_grad).astype(BF16)
    feeds = (reduce_weight_grad, expand_weight_grad)
    feed_parts = parts_of(0, feeds[0].shape, BF16, n, (3, 3, 2), orders[:3]) + parts_of(
        1, feeds[1].shape, BF16, n, (1, 1, 2), (orders[0], orders[1], orders[3])
    )
    feed_recvs = [outer_halving(feeds[part.array], part, n) for part in feed_parts]

    normed_two_grad = scatter(lambda part: dot_nt(part, expand_weight), (hidden_grad,))
    own_upstream = own_rows(cotangent).astype(F32)
    _, second_pull = jax.vjp(layer_norm, middle, feedforward_gain, feedforward_shift)
    middle_grad, second_gain_part, second_shift_part = second_pull(normed_two_grad)
    middle_grad = middle_grad + own_upstream
    branch_grad = gather(middle_grad.astype(BF16))
    attended_grad = dot_nt(branch_grad, output_weight).astype(BF16)
    early = min(EARLY, len(feed_parts))
    joint_grad, feed_sums = attend_back(
        queries, keys, values, attended_grad, exact, inverse, weights, feeds, feed_recvs, feed_parts, early, bits
    )
    output_weight_grad = dot_tn(attended, branch_grad).astype(BF16)
    input_weight_grad = tuple(dot_tn(normed, part).astype(BF16) for part in joint_grad)
    rest = [*input_weight_grad, output_weight_grad]
    fits = [divides(part.shape, part.dtype, n) for part in rest]
    sources, rest_parts = [], []
    for which, part in enumerate(rest):
        if fits[which]:
            rest_parts += parts_of(len(sources), part.shape, part.dtype, n, (1,), (orders[which % 4],))
            sources.append(part)
    rest_recvs = [outer_halving(sources[part.array], part, n) for part in rest_parts]

    def back_through(query_part, key_part, value_part):
        return (
            dot_nt(query_part, stacked_weight[0])
            + dot_nt(key_part, stacked_weight[1])
            + dot_nt(value_part, stacked_weight[2])
        )

    normed_grad = scatter(back_through, tuple(joint_grad))
    _, first_pull = jax.vjp(layer_norm, own_inputs, attention_gain, attention_shift)
    inputs_grad, first_gain_part, first_shift_part = first_pull(normed_grad)
    tokens_gradient = gather_in_order((inputs_grad + middle_grad).astype(BF16))
    result = middle + (scatter(lambda part: dot_nn(part, reduce_weight), (activated,)) + reduce_bias)
    block_out = gather_in_order(result.astype(BF16))

    norm_parts = jnp.stack([first_gain_part, first_shift_part, second_gain_part, second_shift_part])
    norm_parts = norm_parts + swap(norm_parts) if cores == 2 else lax.psum(norm_parts, "tensor")
    small = [
        norm_parts.reshape(-1),
        column_sum(cotangent),
        column_sum(branch_grad),
        column_sum(joint_grad[0]),
        column_sum(joint_grad[2]),
        expand_bias_grad,
    ]
    sizes = [part.shape[0] for part in small]
    table_rows = -(-sum(sizes) // (n * 8 * 128)) * n * 8
    table = jnp.pad(jnp.concatenate(small), (0, table_rows * 128 - sum(sizes))).reshape(table_rows, 128)
    table_parts = parts_of(len(sources), table.shape, F32, n, (1,), orders, outer=False)
    late, summed = rest_sums(
        feed_sums[early:], feed_parts[early:], [*sources, table], rest_recvs, rest_parts + table_parts, bits
    )
    feed_sums = [*feed_sums[:early], *late]

    def whole(array, parts, sums):
        pieces = []
        for part, own in zip(parts, sums):
            if part.array == array:
                pieces += outer_doubling(own, part, n)
        return jnp.concatenate(pieces)

    sums, at = [], 0
    for part, fit in zip(rest, fits):
        sums.append(whole(at, rest_parts, summed) if fit else lax.psum(part, "dp").astype(F32))
        at += int(fit)
    flat = summed[-1].reshape(-1)
    ends = [sum(sizes[: i + 1]) for i in range(len(sizes))]
    parts = [flat[end - size : end] for size, end in zip(sizes, ends)]
    norms = parts[0].reshape(4, -1)
    return (
        block_out,
        tokens_gradient,
        norms[0],
        norms[1],
        jnp.transpose(jnp.stack(sums[:3]), (1, 0, 2)),
        parts[3],
        parts[4],
        sums[3],
        parts[2],
        norms[2],
        norms[3],
        whole(1, feed_parts, feed_sums),
        parts[5],
        whole(0, feed_parts, feed_sums),
        parts[1],
    )


def solution(mesh):
    in_specs = (
        P("dp", None),
        P(),
        P(),
        P(None, None, "tensor"),
        P("tensor"),
        P("tensor"),
        P("tensor", None),
        P(),
        P(),
        P(),
        P(None, "tensor"),
        P("tensor"),
        P("tensor", None),
        P(),
        P("dp", None),
    )
    out_specs = (
        P("dp", None),
        P("dp", None),
        P(),
        P(),
        P(None, None, "tensor"),
        P("tensor"),
        P("tensor"),
        P("tensor", None),
        P(),
        P(),
        P(),
        P(None, "tensor"),
        P("tensor"),
        P("tensor", None),
        P(),
    )
    return jax.shard_map(shards, mesh=mesh, in_specs=in_specs, out_specs=out_specs, check_vma=False)
```

```python
import functools

import jax
import jax.numpy as jnp
from jax import lax
from jax.experimental import pallas as pl
from jax.experimental.pallas import tpu as pltpu
from jax.sharding import PartitionSpec as P


HEAD_DIM = 64
PAIR = 2 * HEAD_DIM
F32 = jnp.float32
BF16 = jnp.bfloat16
EXP_SCALE = 0.125 * 1.4426950408889634


norm_eps = 1e-06


def layer_norm(values, gain, shift):
    center = values - jnp.mean(values, axis=-1, keepdims=True)
    spread = jnp.mean(center * center, axis=-1, keepdims=True)
    return center * lax.rsqrt(spread + norm_eps) * gain + shift


def dot_nn(a, b):
    return lax.dot_general(a, b, (((1,), (0,)), ((), ())), preferred_element_type=F32)


def dot_nt(a, b):
    return lax.dot_general(a, b, (((1,), (1,)), ((), ())), preferred_element_type=F32)


def dot_tn(a, b):
    return lax.dot_general(a, b, (((0,), (0,)), ((), ())), preferred_element_type=F32)


def attend_kernel(q_ref, k_ref, v_ref, out_ref, exact_ref, inverse_ref, weights_ref):
    low_half = lax.broadcasted_iota(jnp.int32, (1, PAIR), 1) < HEAD_DIM
    zero = jnp.zeros((), BF16)
    keys, values, queries = k_ref[...], v_ref[...], q_ref[...]
    mixed, inverses = [], []
    for head in range(2):
        own_keys = jnp.where(low_half if head == 0 else ~low_half, keys, zero)
        scores = dot_nt(queries, own_keys)
        top = jnp.max(scores, axis=1, keepdims=True)
        weights = jnp.exp2((scores - top) * EXP_SCALE)
        inverse = 1.0 / jnp.sum(weights, axis=1, keepdims=True)
        weights = weights.astype(BF16)
        weights_ref[head] = weights
        mixed.append(dot_nn(weights, values) * inverse)
        inverses.append(inverse)
    exact = jnp.where(low_half, mixed[0], mixed[1])
    out_ref[...] = exact.astype(BF16)
    exact_ref[...] = exact
    inverse_ref[...] = jnp.where(low_half, inverses[0], inverses[1])


def attend(queries, keys, values, block=224):
    rows, width = queries.shape
    pairs = width // PAIR
    tile = pl.BlockSpec((block, PAIR), lambda p, i: (i, p))
    whole = pl.BlockSpec((rows, PAIR), lambda p, i: (0, p))
    return pl.pallas_call(
        attend_kernel,
        grid=(pairs, rows // block),
        in_specs=[tile, whole, whole],
        out_specs=[tile, tile, tile, pl.BlockSpec((2, block, rows), lambda p, i: (p, i, 0))],
        out_shape=[
            jax.ShapeDtypeStruct((rows, width), BF16),
            jax.ShapeDtypeStruct((rows, width), F32),
            jax.ShapeDtypeStruct((rows, width), F32),
            jax.ShapeDtypeStruct((2 * pairs, rows, rows), BF16),
        ],
        compiler_params=pltpu.CompilerParams(vmem_limit_bytes=60 << 20),
        cost_estimate=pl.CostEstimate(
            flops=8 * pairs * rows * rows * HEAD_DIM * 4,
            bytes_accessed=4 * pairs * rows * rows,
            transcendentals=2 * pairs * rows * rows,
        ),
        name="attend",
    )(queries, keys, values)


def feed_kernel(n_ref, c_ref, expand_ref, reduce_ref, bias_ref, act_ref, grad_ref, sum_ref, *, chunk):
    @pl.when(pl.program_id(0) == 0)
    def _():
        sum_ref[...] = jnp.zeros_like(sum_ref)

    normed, cotangent = n_ref[...], c_ref[...]
    for first in range(0, expand_ref.shape[1], chunk):
        cols = pl.ds(first, chunk)
        hidden = dot_nn(normed, expand_ref[:, cols]) + bias_ref[:, cols]
        pushed = dot_nt(cotangent, reduce_ref[cols, :])
        share = 0.5 * lax.erf(hidden * ROOT_HALF) + 0.5
        act_ref[:, cols] = (hidden * share).astype(BF16)
        density = jnp.exp2(hidden * hidden * HALF_LOG2E) * NORMAL_PEAK
        grad = (pushed * (share + hidden * density)).astype(BF16)
        grad_ref[:, cols] = grad
        sum_ref[:, cols] += jnp.sum(grad.astype(F32), axis=0, keepdims=True)


def feed(normed, cotangent, expand_weight, reduce_weight, expand_bias, block=224, chunk=256):
    rows, depth = normed.shape
    width = expand_weight.shape[1]
    tile = pl.BlockSpec((block, depth), lambda i: (i, 0))
    out = pl.BlockSpec((block, width), lambda i: (i, 0))

    def whole(shape):
        return pl.BlockSpec(shape, lambda i: (0, 0))

    act, grad, total = pl.pallas_call(
        functools.partial(feed_kernel, chunk=chunk),
        grid=(rows // block,),
        in_specs=[tile, tile, whole((depth, width)), whole((width, depth)), whole((1, width))],
        out_specs=[out, out, whole((1, width))],
        out_shape=[jax.ShapeDtypeStruct((rows, width), BF16)] * 2 + [jax.ShapeDtypeStruct((1, width), F32)],
        compiler_params=pltpu.CompilerParams(vmem_limit_bytes=60 << 20),
        cost_estimate=pl.CostEstimate(
            flops=4 * rows * depth * width, bytes_accessed=8 * rows * (depth + width), transcendentals=rows * width
        ),
        name="feed",
    )(normed, cotangent, expand_weight, reduce_weight, expand_bias.reshape(1, -1))
    return act, grad, total.reshape(-1)


def orders_of(bits):
    if bits == 4:
        return ((0, 1, 2, 3), (1, 0, 2, 3), (2, 0, 1, 3), (2, 1, 0, 3))
    return tuple(tuple((i + j) % bits for j in range(bits)) for i in (0, 1, 2, 3))


class Part:
    def __init__(self, array, first, each, cols, dtype, order, outer):
        self.array, self.first, self.each = array, first, each
        self.cols, self.dtype, self.order, self.outer = cols, dtype, order, outer
        self.inner = order[1:] if outer else order
        self.depth = len(self.inner)
        self.shards = 1 << self.depth
        self.half_rows = self.shards * each


def parts_of(array, shape, dtype, n, shares, orders, outer=True):
    unit = 16 if dtype == BF16 else 8
    units = shape[0] // (n * unit)
    counts = [units * share // sum(shares) for share in shares]
    counts[0] += units - sum(counts)
    parts, first = [], 0
    for count, order in zip(counts, orders):
        if count:
            parts.append(Part(array, first, count * unit, shape[1], dtype, order, outer))
            first += n * count * unit
    return parts


def divides(shape, dtype, n):
    return shape[0] % (n * (16 if dtype == BF16 else 8)) == 0


FEED_PARTS = (
    ((2, 2, 2, 2), ((1, 2, 0, 3), (2, 0, 3, 1), (0, 3, 2, 1), (1, 0, 3, 2))),
    ((2, 1, 1), ((0, 1, 2, 3), (1, 0, 2, 3), (3, 1, 0, 2))),
)
FEED_STEPS = ((2, 0), (5, 0), (0, 0), (1, 0), (5, 1), (4, 0), (3, 0), (1, 1), (2, 1), (6, 0), (3, 1), (4, 1), (5, 2), (2, 2), (1, 2), (0, 1), (0, 2), (1, 3), (5, 3), (6, 1), (3, 2), (4, 2), (6, 2), (3, 3), (1, 4), (6, 3), (0, 3), (6, 4), (4, 3), (2, 3), (2, 4), (3, 4), (1, 5), (4, 4), (6, 5), (0, 4), (5, 4), (2, 5), (0, 5), (3, 5), (4, 5), (5, 5), (3, 6), (6, 6), (1, 6), (4, 6), (5, 6), (0, 6), (2, 6))
FEED_SLOTS = (0, 0, 0, 0, 3, 3, 4, 6, 6, 6, 8, 9, 9, 9, 9, 10, 11, 13, 14, 14, 14, 15, 16, 17, 17, 19, 19, 21, 21, 21, 22, 22, 23, 25, 25, 25, 25, 25, 27, 28, 29, 30, 31, 31, 31, 34, 34, 35, 35)
REST_PARTS = (
    ((1, 1), ((1, 0, 3, 2), (2, 3, 1, 0))),
    ((1,), ((0, 1, 2, 3),)),
    ((1, 1), ((1, 0, 3, 2), (2, 1, 0, 3))),
    ((1, 1), ((0, 2, 1, 3), (1, 0, 3, 2))),
)
REST_STEPS = ((1, 0), (2, 0), (0, 0), (3, 0), (5, 0), (0, 1), (3, 1), (1, 1), (5, 1), (2, 1), (6, 0), (4, 0), (6, 1), (1, 2), (0, 2), (2, 2), (0, 3), (6, 2), (5, 2), (3, 2), (4, 1), (0, 4), (3, 3), (4, 2), (2, 3), (6, 3), (4, 3), (5, 3), (1, 3), (3, 4), (1, 4), (2, 4), (4, 4), (0, 5), (6, 4), (1, 5), (5, 4), (4, 5), (3, 5), (0, 6), (2, 5), (5, 5), (6, 5), (4, 6), (2, 6), (6, 6), (3, 6), (5, 6), (1, 6))


def feed_plan(shapes, n):
    if n == 16:
        parts = [parts_of(i, s, BF16, n, *FEED_PARTS[i]) for i, s in enumerate(shapes)]
        if sum(len(p) for p in parts) == 7:
            return sum(parts, []), FEED_STEPS, FEED_SLOTS
    orders = orders_of(n.bit_length() - 1)
    parts = sum((parts_of(i, s, BF16, n, (1, 1), orders[2 * i : 2 * i + 2]) for i, s in enumerate(shapes)), [])
    steps = [(i, s) for s in range(2 * parts[0].depth + 1) for i in range(len(parts))]
    return parts, steps, None


def rest_plan(shapes, n):
    if n == 16:
        parts = [parts_of(i, s, BF16, n, *REST_PARTS[i]) for i, s in enumerate(shapes)]
        if sum(len(p) for p in parts) == 7:
            return sum(parts, []), REST_STEPS
    orders = orders_of(n.bit_length() - 1)
    parts = sum((parts_of(i, s, BF16, n, (1,), orders[i : i + 1]) for i, s in enumerate(shapes)), [])
    return parts, [(i, s) for s in range(2 * parts[0].depth + 1) for i in range(len(parts))]


def swap_bit(values, bit, n):
    return lax.ppermute(values, "dp", [(j, j ^ (1 << bit)) for j in range(n)])


def bit_of_index(bit):
    return (lax.axis_index("dp") >> bit) & 1


def outer_gift(array, part):
    other = 1 - bit_of_index(part.order[0])
    return lax.dynamic_slice_in_dim(array, part.first + other * part.half_rows, part.half_rows, 0)


def outer_join(own, other, part):
    low = bit_of_index(part.order[0]) == 0
    return [jnp.where(low, own, other).astype(F32), jnp.where(low, other, own).astype(F32)]


class Reduction:
    def __init__(self, parts, bits, bufs, lands, gathers, sems):
        self.parts, self.bits = parts, bits
        self.bufs, self.lands, self.gathers = bufs, lands, gathers
        self.load_sem, self.store_sem, self.send_sem, self.recv_sem = sems
        me = lax.axis_index("dp")
        self.digit = [(me // (1 << b)) % 2 for b in range(bits)]
        self.partner = [me + (1 << b) * (1 - 2 * self.digit[b]) for b in range(bits)]

    def greet(self):
        barrier = pltpu.get_barrier_semaphore()
        for b in range(self.bits):
            pl.semaphore_signal(
                barrier, inc=1, device_id={"dp": self.partner[b]}, device_id_type=pl.DeviceIdType.MESH
            )
        pl.semaphore_wait(barrier, self.bits)

    def rows(self, i, position, base=0):
        part, shard = self.parts[i], 0
        for level, b in enumerate(part.inner):
            flip = (position >> (part.depth - 1 - level)) & 1
            shard = shard + (1 << (part.depth - 1 - level)) * ((1 - self.digit[b]) if flip else self.digit[b])
        return pl.ds(pl.multiple_of(base + shard * part.each, 8), part.each)

    def load(self, i, ref, recv):
        part = self.parts[i]
        base = part.first + (self.digit[part.order[0]] * part.half_rows if part.outer else 0)
        for position in range(part.shards):
            pltpu.make_async_copy(
                ref.at[self.rows(i, position, base), :], self.bufs[i].at[position], self.load_sem.at[2 * i]
            ).start()
            if part.outer:
                pltpu.make_async_copy(
                    recv.at[self.rows(i, position), :], self.lands[i].at[position], self.load_sem.at[2 * i + 1]
                ).start()

    def begin(self, i):
        part, buf, land = self.parts[i], self.bufs[i], self.lands[i]
        pltpu.make_async_copy(buf, buf, self.load_sem.at[2 * i]).wait()
        if part.outer:
            got = land.at[pl.ds(0, part.shards)]
            pltpu.make_async_copy(got, got, self.load_sem.at[2 * i + 1]).wait()
            self.add(i, 0, part.shards, buf)

    def add(self, i, start, count, to):
        buf, land = self.bufs[i], self.lands[i]

        def body(j, carry):
            to[j] = (buf[j].astype(F32) + land[start + j].astype(F32)).astype(buf.dtype)
            return carry

        lax.fori_loop(0, count, body, 0)

    def store(self, i, ref):
        base = 0 if self.parts[i].outer else self.parts[i].first
        for position in range(self.parts[i].shards):
            pltpu.make_async_copy(
                self.gathers[i].at[position], ref.at[self.rows(i, position, base), :], self.store_sem.at[i]
            ).start()

    def store_wait(self, i):
        pltpu.make_async_copy(self.gathers[i], self.gathers[i], self.store_sem.at[i]).wait()

    def exchange(self, i, number):
        part = self.parts[i]
        level = number if number < part.depth else 2 * part.depth - 1 - number
        half = part.shards >> (level + 1)
        if number < part.depth:
            at = (part.shards if part.outer else 0) + part.shards - 2 * half
            source, target = self.bufs[i].at[pl.ds(half, half)], self.lands[i].at[pl.ds(at, half)]
        else:
            source, target = self.gathers[i].at[pl.ds(0, half)], self.gathers[i].at[pl.ds(half, half)]
        k = sum(2 * p.depth for p in self.parts[:i]) + number
        return pltpu.make_async_remote_copy(
            source,
            target,
            self.send_sem.at[k],
            self.recv_sem.at[k],
            device_id={"dp": self.partner[part.inner[level]]},
            device_id_type=pl.DeviceIdType.MESH,
        )

    def finish(self, i, number):
        self.exchange(i, number).wait()
        part = self.parts[i]
        if number < part.depth:
            half = part.shards >> (number + 1)
            at = (part.shards if part.outer else 0) + part.shards - 2 * half
            self.add(i, at, half, self.gathers[i] if number == part.depth - 1 else self.bufs[i])


def buffers(summed, gathered):
    return (
        [pltpu.VMEM((p.shards, p.each, p.cols), p.dtype) for p in summed]
        + [pltpu.VMEM((p.shards * (2 if p.outer else 1) - 1, p.each, p.cols), p.dtype) for p in summed]
        + [pltpu.VMEM((p.shards, p.each, p.cols), p.dtype) for p in gathered]
    )


def semaphores(parts):
    exchanges = sum(2 * p.depth for p in parts)
    return [
        pltpu.SemaphoreType.DMA((2 * len(parts),)),
        pltpu.SemaphoreType.DMA((len(parts),)),
        pltpu.SemaphoreType.DMA((exchanges,)),
        pltpu.SemaphoreType.DMA((exchanges,)),
    ]


def attend_back_kernel(parts, plan, slots, bits, arrays, total, *refs):
    count = len(parts)
    q_ref, k_ref, v_ref, g_ref, o_ref, inverse_ref, weights_ref = refs[:7]
    sources, recvs, refs = refs[7 : 7 + arrays], refs[7 + arrays : 7 + arrays + count], refs[7 + arrays + count :]
    dq_ref, dk_ref, dv_ref = refs[:3]
    results, refs = refs[3 : 3 + count], refs[3 + count :]
    dk_sum, dv_sum = refs[:2]
    refs = refs[2:]
    sums = Reduction(
        parts, bits, refs[:count], refs[count : 2 * count], refs[2 * count : 3 * count], refs[3 * count :]
    )
    step, steps = pl.program_id(1), pl.num_programs(1)
    low_half = lax.broadcasted_iota(jnp.int32, (1, PAIR), 1) < HEAD_DIM
    zero = jnp.zeros((), BF16)
    now = pl.program_id(0) * steps + step

    @pl.when(now == 0)
    def _():
        for i in range(count):
            sums.load(i, sources[parts[i].array], recvs[i])
        sums.greet()

    def advance(i, number):
        if number == 0:
            sums.begin(i)
        else:
            sums.finish(i, number - 1)
        if number < 2 * parts[i].depth:
            sums.exchange(i, number).start()
        else:
            sums.store(i, results[i])

    places = slots or [total * k // len(plan) for k in range(len(plan))]
    for slot in sorted(set(places)):
        if slot < total:

            @pl.when(now == slot)
            def _(slot=slot):
                for event, place in zip(plan, places):
                    if place == slot:
                        advance(*event)

    @pl.when(step == 0)
    def _():
        dk_sum[...] = jnp.zeros_like(dk_sum)
        dv_sum[...] = jnp.zeros_like(dv_sum)

    keys, values, queries = k_ref[...], v_ref[...], q_ref[...]
    grads = (g_ref[...].astype(F32) * inverse_ref[...]).astype(BF16)
    products = grads.astype(F32) * o_ref[...]
    query_grad = None
    for head in range(2):
        own = low_half if head == 0 else ~low_half
        inner = jnp.sum(jnp.where(own, products, 0.0), axis=1, keepdims=True)
        weights = weights_ref[head]
        pushed = dot_nt(grads, jnp.where(own, values, zero))
        score_grad = (weights.astype(F32) * (pushed - inner)).astype(BF16)
        part = dot_nn(score_grad, jnp.where(own, keys, zero))
        query_grad = part if query_grad is None else query_grad + part
        dv_sum[...] += dot_tn(weights, jnp.where(own, grads, zero))
        dk_sum[...] += dot_tn(score_grad, jnp.where(own, queries, zero))
    dq_ref[...] = (query_grad * 0.125).astype(BF16)

    @pl.when(step == steps - 1)
    def _():
        dk_ref[...] = (dk_sum[...] * 0.125).astype(BF16)
        dv_ref[...] = dv_sum[...].astype(BF16)

    @pl.when(now == total - 1)
    def _():
        for event, place in zip(plan, places):
            if place >= total:
                advance(*event)
        for i in range(count):
            sums.store_wait(i)


def attend_back(queries, keys, values, grads, outs, inverse, weights, sources, recvs, plan, bits, block=224):
    parts, plan, slots = plan
    rows, width = queries.shape
    pairs = width // PAIR
    tile = pl.BlockSpec((block, PAIR), lambda p, i: (i, p))
    whole = pl.BlockSpec((rows, PAIR), lambda p, i: (0, p))
    anywhere = pl.BlockSpec(memory_space=pl.ANY)
    results = pl.pallas_call(
        functools.partial(attend_back_kernel, parts, plan, slots, bits, len(sources), pairs * (rows // block)),
        grid=(pairs, rows // block),
        in_specs=[tile, whole, whole, tile, tile, tile, pl.BlockSpec((2, block, rows), lambda p, i: (p, i, 0))]
        + [anywhere] * (len(sources) + len(recvs)),
        out_specs=[tile, whole, whole] + [anywhere] * len(parts),
        out_shape=[jax.ShapeDtypeStruct((rows, width), BF16)] * 3
        + [jax.ShapeDtypeStruct((p.half_rows, p.cols), p.dtype) for p in parts],
        scratch_shapes=[pltpu.VMEM((rows, PAIR), F32)] * 2 + buffers(parts, parts) + semaphores(parts),
        compiler_params=pltpu.CompilerParams(vmem_limit_bytes=60 << 20, collective_id=0, has_side_effects=True),
        cost_estimate=pl.CostEstimate(
            flops=16 * pairs * rows * rows * HEAD_DIM * 4,
            bytes_accessed=4 * pairs * rows * rows,
            transcendentals=0,
        ),
        name="attend_back",
    )(queries, keys, values, grads, outs, inverse, weights, *sources, *recvs)
    return results[:3], results[3:]


def rest_kernel(parts, plan, bits, arrays, *refs):
    count = len(parts)
    sources, refs = refs[:arrays], refs[arrays:]
    outer = [i for i, p in enumerate(parts) if p.outer]
    recvs, refs = dict(zip(outer, refs[: len(outer)])), refs[len(outer) :]
    results, refs = refs[:count], refs[count:]
    sums = Reduction(
        parts, bits, refs[:count], refs[count : 2 * count], refs[2 * count : 3 * count], refs[3 * count :]
    )
    for i in range(count):
        sums.load(i, sources[parts[i].array], recvs.get(i))
    sums.greet()

    def advance(i, number):
        if number == 0:
            sums.begin(i)
        else:
            sums.finish(i, number - 1)
        if number < 2 * parts[i].depth:
            sums.exchange(i, number).start()
        else:
            sums.store(i, results[i])

    for event in plan:
        advance(*event)
    for i in range(count):
        sums.store_wait(i)


def rest_sums(sources, recvs, parts, plan, bits):
    anywhere = pl.BlockSpec(memory_space=pl.ANY)
    shapes = [
        jax.ShapeDtypeStruct((p.half_rows if p.outer else p.first + p.shards * p.each, p.cols), p.dtype)
        for p in parts
    ]
    return pl.pallas_call(
        functools.partial(rest_kernel, parts, plan, bits, len(sources)),
        in_specs=[anywhere] * (len(sources) + len(recvs)),
        out_specs=[anywhere] * len(shapes),
        out_shape=shapes,
        scratch_shapes=buffers(parts, parts) + semaphores(parts),
        compiler_params=pltpu.CompilerParams(vmem_limit_bytes=60 << 20, collective_id=1, has_side_effects=True),
        name="rest_sums",
    )(*sources, *recvs)


ROOT_HALF = 0.7071067811865476
HALF_LOG2E = -0.5 * 1.4426950408889634
NORMAL_PEAK = 0.3989422804014327


def column_sum(values):
    return jnp.sum(values, axis=0, dtype=F32)


def shards(
    tokens,
    attention_gain,
    attention_shift,
    input_weight,
    query_bias,
    value_bias,
    output_weight,
    output_bias,
    feedforward_gain,
    feedforward_shift,
    expand_weight,
    expand_bias,
    reduce_weight,
    reduce_bias,
    cotangent,
):
    rows = tokens.shape[0]
    cores = lax.axis_size("tensor")
    core = lax.axis_index("tensor")
    share = rows // cores
    n = lax.axis_size("dp")
    bits = n.bit_length() - 1
    orders = orders_of(bits)

    if cores == 2:

        def own_first(values):
            own = lax.dynamic_slice_in_dim(values, core * share, share, 0)
            return jnp.concatenate([own, lax.dynamic_slice_in_dim(values, (1 - core) * share, share, 0)])

        def swap(values):
            return lax.ppermute(values, "tensor", [(0, 1), (1, 0)])

        def scatter(product, values):
            other = product(*(v[share:] for v in values)).astype(BF16)
            other = swap(other)
            return product(*(v[:share] for v in values)) + other.astype(F32)

        def gather(values):
            return jnp.concatenate([values, swap(values)])

        def gather_in_order(values):
            other = swap(values)
            first = core == 0
            return jnp.concatenate([jnp.where(first, values, other), jnp.where(first, other, values)])

        first_row = 0
    else:

        def own_first(values):
            return values

        def scatter(product, values):
            return lax.psum_scatter(product(*values).astype(BF16), "tensor", scatter_dimension=0, tiled=True).astype(F32)

        def gather(values):
            return lax.all_gather(values, "tensor", axis=0, tiled=True)

        gather_in_order = gather
        first_row = core * share

    def own_rows(values):
        if cores == 2:
            return values[:share]
        return lax.dynamic_slice_in_dim(values, first_row, share, 0)

    stacked_weight = jnp.transpose(input_weight, (1, 0, 2))
    tokens = own_first(tokens)
    cotangent = own_first(cotangent)
    inputs = tokens.astype(F32)
    normed = layer_norm(inputs, attention_gain, attention_shift).astype(BF16)
    queries = (dot_nn(normed, stacked_weight[0]) + query_bias).astype(BF16)
    keys = dot_nn(normed, stacked_weight[1]).astype(BF16)
    values = (dot_nn(normed, stacked_weight[2]) + value_bias).astype(BF16)
    attended, exact, inverse, weights = attend(queries, keys, values)
    own_inputs = own_rows(tokens).astype(F32)
    middle = own_inputs + scatter(lambda part: dot_nn(part, output_weight), (attended,)) + output_bias
    normed_two = layer_norm(middle, feedforward_gain, feedforward_shift).astype(BF16)
    gathered = gather(normed_two)
    activated, hidden_grad, expand_bias_grad = feed(gathered, cotangent, expand_weight, reduce_weight, expand_bias)
    reduce_weight_grad = dot_tn(activated, cotangent).astype(BF16)
    expand_weight_grad = dot_tn(gathered, hidden_grad).astype(BF16)
    feeds = (reduce_weight_grad, expand_weight_grad)
    feed_parts, feed_steps, feed_slots = feed_plan([grad.shape for grad in feeds], n)
    gifts = [outer_gift(feeds[part.array], part) for part in feed_parts]
    hidden_grad, *gifts = lax.optimization_barrier((hidden_grad, *gifts))
    feed_recvs = [swap_bit(gift, part.order[0], n) for gift, part in zip(gifts, feed_parts)]

    normed_two_grad = scatter(lambda part: dot_nt(part, expand_weight), (hidden_grad,))
    own_upstream = own_rows(cotangent).astype(F32)
    _, second_pull = jax.vjp(layer_norm, middle, feedforward_gain, feedforward_shift)
    middle_grad, second_gain_part, second_shift_part = second_pull(normed_two_grad)
    middle_grad = middle_grad + own_upstream
    branch_grad = gather(middle_grad.astype(BF16))
    attended_grad = dot_nt(branch_grad, output_weight).astype(BF16)
    output_weight_grad = dot_tn(attended, branch_grad).astype(BF16)
    attended_grad, output_weight_grad = lax.optimization_barrier((attended_grad, output_weight_grad))
    joint_grad, feed_sums = attend_back(
        queries,
        keys,
        values,
        attended_grad,
        exact,
        inverse,
        weights,
        feeds,
        feed_recvs,
        (feed_parts, feed_steps, feed_slots),
        bits,
    )
    feed_others = [swap_bit(own, part.order[0], n) for own, part in zip(feed_sums, feed_parts)]
    input_weight_grad = tuple(dot_tn(normed, part).astype(BF16) for part in joint_grad)
    rest = [*input_weight_grad, output_weight_grad]
    fits = [divides(part.shape, part.dtype, n) for part in rest]
    sources = [part for part, fit in zip(rest, fits) if fit]
    rest_parts, rest_steps = rest_plan([part.shape for part in sources], n)
    gifts = [outer_gift(sources[part.array], part) for part in rest_parts]
    *joint_grad, gifts = lax.optimization_barrier((*joint_grad, gifts))
    rest_recvs = [swap_bit(gift, part.order[0], n) for gift, part in zip(gifts, rest_parts)]

    def back_through(query_part, key_part, value_part):
        return (
            dot_nt(query_part, stacked_weight[0])
            + dot_nt(key_part, stacked_weight[1])
            + dot_nt(value_part, stacked_weight[2])
        )

    normed_grad = scatter(back_through, tuple(joint_grad))
    _, first_pull = jax.vjp(layer_norm, own_inputs, attention_gain, attention_shift)
    inputs_grad, first_gain_part, first_shift_part = first_pull(normed_grad)
    tokens_gradient = gather_in_order((inputs_grad + middle_grad).astype(BF16))
    norm_parts = jnp.stack([first_gain_part, first_shift_part, second_gain_part, second_shift_part])
    norm_parts = norm_parts + swap(norm_parts) if cores == 2 else lax.psum(norm_parts, "tensor")
    small = [
        norm_parts.reshape(-1),
        column_sum(cotangent),
        column_sum(branch_grad),
        column_sum(joint_grad[0]),
        column_sum(joint_grad[2]),
        expand_bias_grad,
    ]
    sizes = [part.shape[0] for part in small]
    table_rows = -(-sum(sizes) // (n * 8 * 128)) * n * 8
    table = jnp.pad(jnp.concatenate(small), (0, table_rows * 128 - sum(sizes))).reshape(table_rows, 128)
    table_parts = parts_of(len(sources), table.shape, F32, n, (1,), orders, outer=False)
    steps = list(rest_steps)
    for k in range(2 * bits, -1, -1):
        steps.insert(k * len(steps) // (2 * bits + 1), (len(rest_parts), k))
    summed = rest_sums([*sources, table], rest_recvs, rest_parts + table_parts, steps, bits)
    rest_others = [swap_bit(own, part.order[0], n) for own, part in zip(summed, rest_parts)]
    activated, feed_sums, summed = lax.optimization_barrier((activated, feed_sums, summed))
    update = scatter(lambda part: dot_nn(part, reduce_weight), (activated,))
    result = middle + (update + reduce_bias)
    block_out = gather_in_order(result.astype(BF16))

    def whole(array, parts, sums, others):
        pieces = []
        for part, own, other in zip(parts, sums, others):
            if part.array == array:
                pieces += outer_join(own, other, part)
        return jnp.concatenate(pieces)

    sums, at = [], 0
    for part, fit in zip(rest, fits):
        sums.append(whole(at, rest_parts, summed, rest_others) if fit else lax.psum(part, "dp").astype(F32))
        at += int(fit)
    flat = summed[-1].reshape(-1)
    ends = [sum(sizes[: i + 1]) for i in range(len(sizes))]
    parts = [flat[end - size : end] for size, end in zip(sizes, ends)]
    norms = parts[0].reshape(4, -1)
    return (
        block_out,
        tokens_gradient,
        norms[0],
        norms[1],
        jnp.transpose(jnp.stack(sums[:3]), (1, 0, 2)),
        parts[3],
        parts[4],
        sums[3],
        parts[2],
        norms[2],
        norms[3],
        whole(1, feed_parts, feed_sums, feed_others),
        parts[5],
        whole(0, feed_parts, feed_sums, feed_others),
        parts[1],
    )


def solution(mesh):
    in_specs = (
        P("dp", None),
        P(),
        P(),
        P(None, None, "tensor"),
        P("tensor"),
        P("tensor"),
        P("tensor", None),
        P(),
        P(),
        P(),
        P(None, "tensor"),
        P("tensor"),
        P("tensor", None),
        P(),
        P("dp", None),
    )
    out_specs = (
        P("dp", None),
        P("dp", None),
        P(),
        P(),
        P(None, None, "tensor"),
        P("tensor"),
        P("tensor"),
        P("tensor", None),
        P(),
        P(),
        P(),
        P(None, "tensor"),
        P("tensor"),
        P("tensor", None),
        P(),
    )

    return jax.shard_map(shards, mesh=mesh, in_specs=in_specs, out_specs=out_specs, check_vma=False)
```

```python
import functools

import jax
import jax.numpy as jnp
from jax import lax
from jax.experimental import pallas as pl
from jax.experimental.pallas import tpu as pltpu
from jax.sharding import PartitionSpec as P


HEAD_DIM = 64
PAIR = 2 * HEAD_DIM
F32 = jnp.float32
BF16 = jnp.bfloat16
EXP_SCALE = 0.125 * 1.4426950408889634


norm_eps = 1e-06


def layer_norm(values, gain, shift):
    center = values - jnp.mean(values, axis=-1, keepdims=True)
    spread = jnp.mean(center * center, axis=-1, keepdims=True)
    return center * lax.rsqrt(spread + norm_eps) * gain + shift


def dot_nn(a, b):
    return lax.dot_general(a, b, (((1,), (0,)), ((), ())), preferred_element_type=F32)


def dot_nt(a, b):
    return lax.dot_general(a, b, (((1,), (1,)), ((), ())), preferred_element_type=F32)


def dot_tn(a, b):
    return lax.dot_general(a, b, (((0,), (0,)), ((), ())), preferred_element_type=F32)


def attend_kernel(q_ref, k_ref, v_ref, out_ref, exact_ref, inverse_ref, weights_ref):
    low_half = lax.broadcasted_iota(jnp.int32, (1, PAIR), 1) < HEAD_DIM
    zero = jnp.zeros((), BF16)
    keys, values, queries = k_ref[...], v_ref[...], q_ref[...]
    mixed, inverses = [], []
    for head in range(2):
        own_keys = jnp.where(low_half if head == 0 else ~low_half, keys, zero)
        scores = dot_nt(queries, own_keys)
        top = jnp.max(scores, axis=1, keepdims=True)
        weights = jnp.exp2((scores - top) * EXP_SCALE)
        inverse = 1.0 / jnp.sum(weights, axis=1, keepdims=True)
        weights = weights.astype(BF16)
        weights_ref[head] = weights
        mixed.append(dot_nn(weights, values) * inverse)
        inverses.append(inverse)
    exact = jnp.where(low_half, mixed[0], mixed[1])
    out_ref[...] = exact.astype(BF16)
    exact_ref[...] = exact
    inverse_ref[...] = jnp.where(low_half, inverses[0], inverses[1])


def attend(queries, keys, values, block=224):
    rows, width = queries.shape
    pairs = width // PAIR
    tile = pl.BlockSpec((block, PAIR), lambda p, i: (i, p))
    whole = pl.BlockSpec((rows, PAIR), lambda p, i: (0, p))
    return pl.pallas_call(
        attend_kernel,
        grid=(pairs, rows // block),
        in_specs=[tile, whole, whole],
        out_specs=[tile, tile, tile, pl.BlockSpec((2, block, rows), lambda p, i: (p, i, 0))],
        out_shape=[
            jax.ShapeDtypeStruct((rows, width), BF16),
            jax.ShapeDtypeStruct((rows, width), F32),
            jax.ShapeDtypeStruct((rows, width), F32),
            jax.ShapeDtypeStruct((2 * pairs, rows, rows), BF16),
        ],
        compiler_params=pltpu.CompilerParams(vmem_limit_bytes=60 << 20),
        cost_estimate=pl.CostEstimate(
            flops=8 * pairs * rows * rows * HEAD_DIM * 4,
            bytes_accessed=4 * pairs * rows * rows,
            transcendentals=2 * pairs * rows * rows,
        ),
        name="attend",
    )(queries, keys, values)


def feed_kernel(n_ref, c_ref, expand_ref, reduce_ref, bias_ref, act_ref, grad_ref, sum_ref, *, chunk):
    @pl.when(pl.program_id(0) == 0)
    def _():
        sum_ref[...] = jnp.zeros_like(sum_ref)

    normed, cotangent = n_ref[...], c_ref[...]
    for first in range(0, expand_ref.shape[1], chunk):
        cols = pl.ds(first, chunk)
        hidden = dot_nn(normed, expand_ref[:, cols]) + bias_ref[:, cols]
        pushed = dot_nt(cotangent, reduce_ref[cols, :])
        share = 0.5 * lax.erf(hidden * ROOT_HALF) + 0.5
        act_ref[:, cols] = (hidden * share).astype(BF16)
        density = jnp.exp2(hidden * hidden * HALF_LOG2E) * NORMAL_PEAK
        grad = (pushed * (share + hidden * density)).astype(BF16)
        grad_ref[:, cols] = grad
        sum_ref[:, cols] += jnp.sum(grad.astype(F32), axis=0, keepdims=True)


def feed(normed, cotangent, expand_weight, reduce_weight, expand_bias, block=224, chunk=256):
    rows, depth = normed.shape
    width = expand_weight.shape[1]
    tile = pl.BlockSpec((block, depth), lambda i: (i, 0))
    out = pl.BlockSpec((block, width), lambda i: (i, 0))

    def whole(shape):
        return pl.BlockSpec(shape, lambda i: (0, 0))

    act, grad, total = pl.pallas_call(
        functools.partial(feed_kernel, chunk=chunk),
        grid=(rows // block,),
        in_specs=[tile, tile, whole((depth, width)), whole((width, depth)), whole((1, width))],
        out_specs=[out, out, whole((1, width))],
        out_shape=[jax.ShapeDtypeStruct((rows, width), BF16)] * 2 + [jax.ShapeDtypeStruct((1, width), F32)],
        compiler_params=pltpu.CompilerParams(vmem_limit_bytes=60 << 20),
        cost_estimate=pl.CostEstimate(
            flops=4 * rows * depth * width, bytes_accessed=8 * rows * (depth + width), transcendentals=rows * width
        ),
        name="feed",
    )(normed, cotangent, expand_weight, reduce_weight, expand_bias.reshape(1, -1))
    return act, grad, total.reshape(-1)


def orders_of(bits):
    if bits == 4:
        return ((0, 1, 2, 3), (1, 0, 2, 3), (2, 0, 1, 3), (2, 1, 0, 3))
    return tuple(tuple((i + j) % bits for j in range(bits)) for i in (0, 1, 2, 3))


class Part:
    def __init__(self, array, first, each, cols, dtype, order, outer):
        self.array, self.first, self.each = array, first, each
        self.cols, self.dtype, self.order, self.outer = cols, dtype, order, outer
        self.inner = order[1:] if outer else order
        self.depth = len(self.inner)
        self.shards = 1 << self.depth
        self.half_rows = self.shards * each


def parts_of(array, shape, dtype, n, shares, orders, outer=True):
    unit = 16 if dtype == BF16 else 8
    units = shape[0] // (n * unit)
    counts = [units * share // sum(shares) for share in shares]
    counts[0] += units - sum(counts)
    parts, first = [], 0
    for count, order in zip(counts, orders):
        if count:
            parts.append(Part(array, first, count * unit, shape[1], dtype, order, outer))
            first += n * count * unit
    return parts


def divides(shape, dtype, n):
    return shape[0] % (n * (16 if dtype == BF16 else 8)) == 0


FEED_PARTS = (
    ((2, 2, 2, 2), ((1, 2, 0, 3), (2, 0, 3, 1), (0, 3, 2, 1), (1, 0, 3, 2))),
    ((2, 1, 1), ((0, 1, 2, 3), (1, 0, 2, 3), (3, 1, 0, 2))),
)
FEED_STEPS = ((2, 0), (5, 0), (0, 0), (1, 0), (5, 1), (4, 0), (3, 0), (1, 1), (2, 1), (6, 0), (3, 1), (4, 1), (5, 2), (2, 2), (1, 2), (0, 1), (0, 2), (1, 3), (5, 3), (6, 1), (3, 2), (4, 2), (6, 2), (3, 3), (1, 4), (6, 3), (0, 3), (6, 4), (4, 3), (2, 3), (2, 4), (3, 4), (1, 5), (4, 4), (6, 5), (0, 4), (5, 4), (2, 5), (0, 5), (3, 5), (4, 5), (5, 5), (3, 6), (6, 6), (1, 6), (4, 6), (5, 6), (0, 6), (2, 6))
FEED_SLOTS = (0, 0, 0, 0, 3, 3, 4, 6, 6, 6, 8, 9, 9, 9, 9, 10, 11, 13, 14, 14, 14, 15, 16, 17, 17, 19, 19, 21, 21, 21, 22, 22, 23, 25, 25, 25, 25, 25, 27, 28, 29, 30, 31, 31, 31, 34, 34, 35, 35)
REST_PARTS = (
    ((2, 2, 4, 2, 2), ((1, 0, 3, 2), (2, 3, 1, 0), (0, 1, 2, 3), (1, 0, 3, 2), (2, 1, 0, 3))),
    ((1, 1), ((0, 2, 1, 3), (1, 0, 3, 2))),
)
REST_STEPS = ((1, 0), (2, 0), (0, 0), (3, 0), (5, 0), (0, 1), (3, 1), (1, 1), (5, 1), (2, 1), (6, 0), (4, 0), (6, 1), (1, 2), (0, 2), (2, 2), (0, 3), (6, 2), (5, 2), (3, 2), (4, 1), (0, 4), (3, 3), (4, 2), (2, 3), (6, 3), (4, 3), (5, 3), (1, 3), (3, 4), (1, 4), (2, 4), (4, 4), (0, 5), (6, 4), (1, 5), (5, 4), (4, 5), (3, 5), (0, 6), (2, 5), (5, 5), (6, 5), (4, 6), (2, 6), (6, 6), (3, 6), (5, 6), (1, 6))


def feed_plan(shapes, n):
    if n == 16:
        parts = [parts_of(i, s, BF16, n, *FEED_PARTS[i]) for i, s in enumerate(shapes)]
        if sum(len(p) for p in parts) == 7:
            return sum(parts, []), FEED_STEPS, FEED_SLOTS
    orders = orders_of(n.bit_length() - 1)
    parts = sum((parts_of(i, s, BF16, n, (1, 1), orders[2 * i : 2 * i + 2]) for i, s in enumerate(shapes)), [])
    steps = [(i, s) for s in range(2 * parts[0].depth + 1) for i in range(len(parts))]
    return parts, steps, None


def rest_plan(shapes, n):
    if n == 16:
        parts = [parts_of(i, s, BF16, n, *REST_PARTS[i]) for i, s in enumerate(shapes)]
        if sum(len(p) for p in parts) == 7:
            return sum(parts, []), REST_STEPS
    orders = orders_of(n.bit_length() - 1)
    parts = sum((parts_of(i, s, BF16, n, (1,), orders[i : i + 1]) for i, s in enumerate(shapes)), [])
    return parts, [(i, s) for s in range(2 * parts[0].depth + 1) for i in range(len(parts))]


def swap_bit(values, bit, n):
    return lax.ppermute(values, "dp", [(j, j ^ (1 << bit)) for j in range(n)])


def bit_of_index(bit):
    return (lax.axis_index("dp") >> bit) & 1


def outer_gift(array, part):
    other = 1 - bit_of_index(part.order[0])
    return lax.dynamic_slice_in_dim(array, part.first + other * part.half_rows, part.half_rows, 0)


def join_kernel(parts, *refs):
    count = len(parts)
    halves, outs = refs[: 2 * count], refs[2 * count : -2 - 4 * count]
    takes, gives = refs[-2 - 4 * count : -2 - 2 * count], refs[-2 - 2 * count : -2]
    take_sem, give_sem = refs[-2:]
    copies = []
    for k in range(2 * count):
        pltpu.make_async_copy(halves[k], takes[k], take_sem.at[k]).start()
    me = lax.axis_index("dp")
    for k in range(2 * count):
        part = parts[k // 2]
        digit = (me // (1 << part.order[0])) % 2
        place = digit if k % 2 == 0 else 1 - digit
        pltpu.make_async_copy(halves[k], takes[k], take_sem.at[k]).wait()
        gives[k][...] = takes[k][...].astype(F32)
        rows = pl.ds(pl.multiple_of(part.first + place * part.half_rows, 8), part.half_rows)
        copies.append(pltpu.make_async_copy(gives[k], outs[part.array].at[rows, :], give_sem.at[k]))
        copies[-1].start()
    for copy in copies:
        copy.wait()


def join(parts, owns, others, shapes):
    halves = [half for pair in zip(owns, others) for half in pair]
    anywhere = pl.BlockSpec(memory_space=pl.ANY)
    takes = [pltpu.VMEM(half.shape, half.dtype) for half in halves]
    gives = [pltpu.VMEM(half.shape, F32) for half in halves]
    size = sum(shape[0] * shape[1] for shape in shapes)
    return pl.pallas_call(
        functools.partial(join_kernel, parts),
        in_specs=[anywhere] * len(halves),
        out_specs=[anywhere] * len(shapes),
        out_shape=[jax.ShapeDtypeStruct(shape, F32) for shape in shapes],
        scratch_shapes=takes
        + gives
        + [pltpu.SemaphoreType.DMA((len(halves),))] * 2,
        compiler_params=pltpu.CompilerParams(vmem_limit_bytes=60 << 20),
        cost_estimate=pl.CostEstimate(flops=size, bytes_accessed=6 * size, transcendentals=0),
        name="join",
    )(*halves)


class Reduction:
    def __init__(self, parts, bits, bufs, lands, gathers, sems):
        self.parts, self.bits = parts, bits
        self.bufs, self.lands, self.gathers = bufs, lands, gathers
        self.load_sem, self.store_sem, self.send_sem, self.recv_sem = sems
        me = lax.axis_index("dp")
        self.digit = [(me // (1 << b)) % 2 for b in range(bits)]
        self.partner = [me + (1 << b) * (1 - 2 * self.digit[b]) for b in range(bits)]

    def greet(self):
        barrier = pltpu.get_barrier_semaphore()
        for b in range(self.bits):
            pl.semaphore_signal(
                barrier, inc=1, device_id={"dp": self.partner[b]}, device_id_type=pl.DeviceIdType.MESH
            )
        pl.semaphore_wait(barrier, self.bits)

    def rows(self, i, position, base=0):
        part, shard = self.parts[i], 0
        for level, b in enumerate(part.inner):
            flip = (position >> (part.depth - 1 - level)) & 1
            shard = shard + (1 << (part.depth - 1 - level)) * ((1 - self.digit[b]) if flip else self.digit[b])
        return pl.ds(pl.multiple_of(base + shard * part.each, 8), part.each)

    def load(self, i, ref, recv):
        part = self.parts[i]
        base = part.first + (self.digit[part.order[0]] * part.half_rows if part.outer else 0)
        for position in range(part.shards):
            pltpu.make_async_copy(
                ref.at[self.rows(i, position, base), :], self.bufs[i].at[position], self.load_sem.at[2 * i]
            ).start()
            if part.outer:
                pltpu.make_async_copy(
                    recv.at[self.rows(i, position), :], self.lands[i].at[position], self.load_sem.at[2 * i + 1]
                ).start()

    def begin(self, i):
        part, buf, land = self.parts[i], self.bufs[i], self.lands[i]
        pltpu.make_async_copy(buf, buf, self.load_sem.at[2 * i]).wait()
        if part.outer:
            got = land.at[pl.ds(0, part.shards)]
            pltpu.make_async_copy(got, got, self.load_sem.at[2 * i + 1]).wait()
            self.add(i, 0, part.shards, buf)

    def add(self, i, start, count, to):
        buf, land = self.bufs[i], self.lands[i]

        def body(j, carry):
            to[j] = (buf[j].astype(F32) + land[start + j].astype(F32)).astype(buf.dtype)
            return carry

        lax.fori_loop(0, count, body, 0)

    def store(self, i, ref):
        base = 0 if self.parts[i].outer else self.parts[i].first
        for position in range(self.parts[i].shards):
            pltpu.make_async_copy(
                self.gathers[i].at[position], ref.at[self.rows(i, position, base), :], self.store_sem.at[i]
            ).start()

    def store_wait(self, i):
        pltpu.make_async_copy(self.gathers[i], self.gathers[i], self.store_sem.at[i]).wait()

    def exchange(self, i, number):
        part = self.parts[i]
        level = number if number < part.depth else 2 * part.depth - 1 - number
        half = part.shards >> (level + 1)
        if number < part.depth:
            at = (part.shards if part.outer else 0) + part.shards - 2 * half
            source, target = self.bufs[i].at[pl.ds(half, half)], self.lands[i].at[pl.ds(at, half)]
        else:
            source, target = self.gathers[i].at[pl.ds(0, half)], self.gathers[i].at[pl.ds(half, half)]
        k = sum(2 * p.depth for p in self.parts[:i]) + number
        return pltpu.make_async_remote_copy(
            source,
            target,
            self.send_sem.at[k],
            self.recv_sem.at[k],
            device_id={"dp": self.partner[part.inner[level]]},
            device_id_type=pl.DeviceIdType.MESH,
        )

    def finish(self, i, number):
        self.exchange(i, number).wait()
        part = self.parts[i]
        if number < part.depth:
            half = part.shards >> (number + 1)
            at = (part.shards if part.outer else 0) + part.shards - 2 * half
            self.add(i, at, half, self.gathers[i] if number == part.depth - 1 else self.bufs[i])


def buffers(summed, gathered):
    return (
        [pltpu.VMEM((p.shards, p.each, p.cols), p.dtype) for p in summed]
        + [pltpu.VMEM((p.shards * (2 if p.outer else 1) - 1, p.each, p.cols), p.dtype) for p in summed]
        + [pltpu.VMEM((p.shards, p.each, p.cols), p.dtype) for p in gathered]
    )


def semaphores(parts):
    exchanges = sum(2 * p.depth for p in parts)
    return [
        pltpu.SemaphoreType.DMA((2 * len(parts),)),
        pltpu.SemaphoreType.DMA((len(parts),)),
        pltpu.SemaphoreType.DMA((exchanges,)),
        pltpu.SemaphoreType.DMA((exchanges,)),
    ]


def attend_back_kernel(parts, plan, slots, bits, arrays, total, *refs):
    count = len(parts)
    q_ref, k_ref, v_ref, o_ref, inverse_ref, weights_ref, branch_ref, ow_ref, att_ref, normed_ref = refs[:10]
    sources, recvs, refs = refs[10 : 10 + arrays], refs[10 + arrays : 10 + arrays + count], refs[10 + arrays + count :]
    dq_ref, dk_ref, dv_ref, dow_ref, diw_ref = refs[:5]
    results, refs = refs[5 : 5 + count], refs[5 + count :]
    dk_sum, dv_sum, g_ref = refs[:3]
    refs = refs[3:]
    sums = Reduction(
        parts, bits, refs[:count], refs[count : 2 * count], refs[2 * count : 3 * count], refs[3 * count :]
    )
    step, steps = pl.program_id(1), pl.num_programs(1)
    low_half = lax.broadcasted_iota(jnp.int32, (1, PAIR), 1) < HEAD_DIM
    zero = jnp.zeros((), BF16)
    now = pl.program_id(0) * steps + step

    @pl.when(now == 0)
    def _():
        for i in range(count):
            sums.load(i, sources[parts[i].array], recvs[i])
        sums.greet()

    def advance(i, number):
        if number == 0:
            sums.begin(i)
        else:
            sums.finish(i, number - 1)
        if number < 2 * parts[i].depth:
            sums.exchange(i, number).start()
        else:
            sums.store(i, results[i])

    places = slots or [total * k // len(plan) for k in range(len(plan))]
    for slot in sorted(set(places)):
        if slot < total:

            @pl.when(now == slot)
            def _(slot=slot):
                for event, place in zip(plan, places):
                    if place == slot:
                        advance(*event)

    @pl.when(step == 0)
    def _():
        dk_sum[...] = jnp.zeros_like(dk_sum)
        dv_sum[...] = jnp.zeros_like(dv_sum)
        branch = branch_ref[...]
        g_ref[...] = dot_nt(branch, ow_ref[...]).astype(BF16)
        dow_ref[...] = dot_tn(att_ref[...], branch).astype(BF16)

    keys, values, queries = k_ref[...], v_ref[...], q_ref[...]
    block = queries.shape[0]
    mine = pl.ds(pl.multiple_of(step * block, block), block)
    grads = (g_ref[mine, :].astype(F32) * inverse_ref[...]).astype(BF16)
    products = grads.astype(F32) * o_ref[...]
    query_grad = None
    for head in range(2):
        own = low_half if head == 0 else ~low_half
        inner = jnp.sum(jnp.where(own, products, 0.0), axis=1, keepdims=True)
        weights = weights_ref[head]
        pushed = dot_nt(grads, jnp.where(own, values, zero))
        score_grad = (weights.astype(F32) * (pushed - inner)).astype(BF16)
        part = dot_nn(score_grad, jnp.where(own, keys, zero))
        query_grad = part if query_grad is None else query_grad + part
        dv_sum[...] += dot_tn(weights, jnp.where(own, grads, zero))
        dk_sum[...] += dot_tn(score_grad, jnp.where(own, queries, zero))
    dq_ref[mine, :] = (query_grad * 0.125).astype(BF16)

    @pl.when(step == steps - 1)
    def _():
        dk_ref[...] = (dk_sum[...] * 0.125).astype(BF16)
        dv_ref[...] = dv_sum[...].astype(BF16)
        joint = jnp.concatenate([dq_ref[...], dk_ref[...], dv_ref[...]], axis=1)
        product = dot_tn(normed_ref[...], joint).astype(BF16)
        for c in range(3):
            diw_ref[c] = product[:, c * PAIR : (c + 1) * PAIR]

    @pl.when(now == total - 1)
    def _():
        for event, place in zip(plan, places):
            if place >= total:
                advance(*event)
        for i in range(count):
            sums.store_wait(i)


def attend_back(queries, keys, values, outs, inverse, weights, branch, output_weight, attended, normed, sources, recvs, plan, bits, block=224):
    parts, plan, slots = plan
    rows, width = queries.shape
    pairs = width // PAIR
    tile = pl.BlockSpec((block, PAIR), lambda p, i: (i, p))
    whole = pl.BlockSpec((rows, PAIR), lambda p, i: (0, p))
    depth = branch.shape[1]
    all_rows = pl.BlockSpec((rows, depth), lambda p, i: (0, 0), pipeline_mode=pl.Buffered(1))
    heads = pl.BlockSpec((PAIR, depth), lambda p, i: (p, 0))
    anywhere = pl.BlockSpec(memory_space=pl.ANY)
    results = pl.pallas_call(
        functools.partial(attend_back_kernel, parts, plan, slots, bits, len(sources), pairs * (rows // block)),
        grid=(pairs, rows // block),
        in_specs=[tile, whole, whole, tile, tile, pl.BlockSpec((2, block, rows), lambda p, i: (p, i, 0))]
        + [all_rows, heads, whole, all_rows]
        + [anywhere] * (len(sources) + len(recvs)),
        out_specs=[whole, whole, whole, heads, pl.BlockSpec((3, depth, PAIR), lambda p, i: (0, 0, p))]
        + [anywhere] * len(parts),
        out_shape=[jax.ShapeDtypeStruct((rows, width), BF16)] * 3
        + [jax.ShapeDtypeStruct((width, depth), BF16), jax.ShapeDtypeStruct((3, depth, width), BF16)]
        + [jax.ShapeDtypeStruct((p.half_rows, p.cols), p.dtype) for p in parts],
        scratch_shapes=[pltpu.VMEM((rows, PAIR), F32)] * 2
        + [pltpu.VMEM((rows, PAIR), BF16)]
        + buffers(parts, parts) + semaphores(parts),
        compiler_params=pltpu.CompilerParams(vmem_limit_bytes=60 << 20, collective_id=0, has_side_effects=True),
        cost_estimate=pl.CostEstimate(
            flops=16 * pairs * rows * rows * HEAD_DIM * 4,
            bytes_accessed=4 * pairs * rows * rows,
            transcendentals=0,
        ),
        name="attend_back",
    )(queries, keys, values, outs, inverse, weights, branch, output_weight, attended, normed, *sources, *recvs)
    return results[:3], results[3], results[4], results[5:]


def rest_kernel(parts, plan, bits, arrays, *refs):
    count = len(parts)
    sources, refs = refs[:arrays], refs[arrays:]
    outer = [i for i, p in enumerate(parts) if p.outer]
    recvs, refs = dict(zip(outer, refs[: len(outer)])), refs[len(outer) :]
    results, refs = refs[:count], refs[count:]
    sums = Reduction(
        parts, bits, refs[:count], refs[count : 2 * count], refs[2 * count : 3 * count], refs[3 * count :]
    )
    for i in range(count):
        sums.load(i, sources[parts[i].array], recvs.get(i))
    sums.greet()

    def advance(i, number):
        if number == 0:
            sums.begin(i)
        else:
            sums.finish(i, number - 1)
        if number < 2 * parts[i].depth:
            sums.exchange(i, number).start()
        else:
            sums.store(i, results[i])

    for event in plan:
        advance(*event)
    for i in range(count):
        sums.store_wait(i)


def rest_sums(sources, recvs, parts, plan, bits):
    anywhere = pl.BlockSpec(memory_space=pl.ANY)
    shapes = [
        jax.ShapeDtypeStruct((p.half_rows if p.outer else p.first + p.shards * p.each, p.cols), p.dtype)
        for p in parts
    ]
    return pl.pallas_call(
        functools.partial(rest_kernel, parts, plan, bits, len(sources)),
        in_specs=[anywhere] * (len(sources) + len(recvs)),
        out_specs=[anywhere] * len(shapes),
        out_shape=shapes,
        scratch_shapes=buffers(parts, parts) + semaphores(parts),
        compiler_params=pltpu.CompilerParams(vmem_limit_bytes=60 << 20, collective_id=1, has_side_effects=True),
        name="rest_sums",
    )(*sources, *recvs)


ROOT_HALF = 0.7071067811865476
HALF_LOG2E = -0.5 * 1.4426950408889634
NORMAL_PEAK = 0.3989422804014327


def column_sum(values):
    return jnp.sum(values, axis=0, dtype=F32)


def shards(
    tokens,
    attention_gain,
    attention_shift,
    input_weight,
    query_bias,
    value_bias,
    output_weight,
    output_bias,
    feedforward_gain,
    feedforward_shift,
    expand_weight,
    expand_bias,
    reduce_weight,
    reduce_bias,
    cotangent,
):
    rows = tokens.shape[0]
    cores = lax.axis_size("tensor")
    core = lax.axis_index("tensor")
    share = rows // cores
    n = lax.axis_size("dp")
    bits = n.bit_length() - 1
    orders = orders_of(bits)

    if cores == 2:

        def own_first(values):
            own = lax.dynamic_slice_in_dim(values, core * share, share, 0)
            return jnp.concatenate([own, lax.dynamic_slice_in_dim(values, (1 - core) * share, share, 0)])

        def swap(values):
            return lax.ppermute(values, "tensor", [(0, 1), (1, 0)])

        def scatter(product, values):
            other = product(*(v[share:] for v in values)).astype(BF16)
            other = swap(other)
            return product(*(v[:share] for v in values)) + other.astype(F32)

        def gather(values):
            return jnp.concatenate([values, swap(values)])

        def gather_in_order(values):
            other = swap(values)
            first = core == 0
            return jnp.concatenate([jnp.where(first, values, other), jnp.where(first, other, values)])

        first_row = 0
    else:

        def own_first(values):
            return values

        def scatter(product, values):
            return lax.psum_scatter(product(*values).astype(BF16), "tensor", scatter_dimension=0, tiled=True).astype(F32)

        def gather(values):
            return lax.all_gather(values, "tensor", axis=0, tiled=True)

        gather_in_order = gather
        first_row = core * share

    def own_rows(values):
        if cores == 2:
            return values[:share]
        return lax.dynamic_slice_in_dim(values, first_row, share, 0)

    stacked_weight = jnp.transpose(input_weight, (1, 0, 2))
    tokens = own_first(tokens)
    cotangent = own_first(cotangent)
    inputs = tokens.astype(F32)
    normed = layer_norm(inputs, attention_gain, attention_shift).astype(BF16)
    queries = (dot_nn(normed, stacked_weight[0]) + query_bias).astype(BF16)
    keys = dot_nn(normed, stacked_weight[1]).astype(BF16)
    values = (dot_nn(normed, stacked_weight[2]) + value_bias).astype(BF16)
    attended, exact, inverse, weights = attend(queries, keys, values)
    own_inputs = own_rows(tokens).astype(F32)
    middle = own_inputs + scatter(lambda part: dot_nn(part, output_weight), (attended,)) + output_bias
    normed_two = layer_norm(middle, feedforward_gain, feedforward_shift).astype(BF16)
    gathered = gather(normed_two)
    activated, hidden_grad, expand_bias_grad = feed(gathered, cotangent, expand_weight, reduce_weight, expand_bias)
    reduce_weight_grad = dot_tn(activated, cotangent).astype(BF16)
    expand_weight_grad = dot_tn(gathered, hidden_grad).astype(BF16)
    feeds = (reduce_weight_grad, expand_weight_grad)
    feed_parts, feed_steps, feed_slots = feed_plan([grad.shape for grad in feeds], n)
    gifts = [outer_gift(feeds[part.array], part) for part in feed_parts]
    hidden_grad, *gifts = lax.optimization_barrier((hidden_grad, *gifts))
    feed_recvs = [swap_bit(gift, part.order[0], n) for gift, part in zip(gifts, feed_parts)]

    normed_two_grad = scatter(lambda part: dot_nt(part, expand_weight), (hidden_grad,))
    own_upstream = own_rows(cotangent).astype(F32)
    _, second_pull = jax.vjp(layer_norm, middle, feedforward_gain, feedforward_shift)
    middle_grad, second_gain_part, second_shift_part = second_pull(normed_two_grad)
    middle_grad = middle_grad + own_upstream
    branch_grad = gather(middle_grad.astype(BF16))
    joint_grad, output_weight_grad, input_weight_grad, feed_sums = attend_back(
        queries,
        keys,
        values,
        exact,
        inverse,
        weights,
        branch_grad,
        output_weight,
        attended,
        normed,
        feeds,
        feed_recvs,
        (feed_parts, feed_steps, feed_slots),
        bits,
    )
    rest = [input_weight_grad.reshape(-1, input_weight_grad.shape[2]), output_weight_grad]
    fits = [divides(part.shape, part.dtype, n) for part in rest]
    sources = [part for part, fit in zip(rest, fits) if fit]
    rest_parts, rest_steps = rest_plan([part.shape for part in sources], n)
    gifts = [outer_gift(sources[part.array], part) for part in rest_parts]
    *joint_grad, activated, feed_sums, gifts = lax.optimization_barrier((*joint_grad, activated, feed_sums, gifts))
    rest_recvs = [swap_bit(gift, part.order[0], n) for gift, part in zip(gifts, rest_parts)]
    feed_others = [swap_bit(own, part.order[0], n) for own, part in zip(feed_sums, feed_parts)]

    def back_through(query_part, key_part, value_part):
        return (
            dot_nt(query_part, stacked_weight[0])
            + dot_nt(key_part, stacked_weight[1])
            + dot_nt(value_part, stacked_weight[2])
        )

    normed_grad = scatter(back_through, tuple(joint_grad))
    _, first_pull = jax.vjp(layer_norm, own_inputs, attention_gain, attention_shift)
    inputs_grad, first_gain_part, first_shift_part = first_pull(normed_grad)
    tokens_gradient = gather_in_order((inputs_grad + middle_grad).astype(BF16))
    update = scatter(lambda part: dot_nn(part, reduce_weight), (activated,))
    result = middle + (update + reduce_bias)
    block_out = gather_in_order(result.astype(BF16))
    norm_parts = jnp.stack([first_gain_part, first_shift_part, second_gain_part, second_shift_part])
    norm_parts = norm_parts + swap(norm_parts) if cores == 2 else lax.psum(norm_parts, "tensor")
    small = [
        norm_parts.reshape(-1),
        column_sum(cotangent),
        column_sum(branch_grad),
        column_sum(joint_grad[0]),
        column_sum(joint_grad[2]),
        expand_bias_grad,
    ]
    sizes = [part.shape[0] for part in small]
    table_rows = -(-sum(sizes) // (n * 8 * 128)) * n * 8
    table = jnp.pad(jnp.concatenate(small), (0, table_rows * 128 - sum(sizes))).reshape(table_rows, 128)
    table_parts = parts_of(len(sources), table.shape, F32, n, (1,), orders, outer=False)
    steps = list(rest_steps)
    for k in range(2 * bits, -1, -1):
        steps.insert(k * len(steps) // (2 * bits + 1), (len(rest_parts), k))
    summed = rest_sums([*sources, table], rest_recvs, rest_parts + table_parts, steps, bits)
    rest_others = [swap_bit(own, part.order[0], n) for own, part in zip(summed, rest_parts)]
    feed_sums, summed = lax.optimization_barrier((feed_sums, summed))
    reduce_total, expand_total = join(feed_parts, feed_sums, feed_others, [grad.shape for grad in feeds])
    joined = list(join(rest_parts, summed[:-1], rest_others, [part.shape for part in sources]))
    sums = [joined.pop(0) if fit else lax.psum(part, "dp").astype(F32) for part, fit in zip(rest, fits)]
    flat = summed[-1].reshape(-1)
    ends = [sum(sizes[: i + 1]) for i in range(len(sizes))]
    parts = [flat[end - size : end] for size, end in zip(sizes, ends)]
    norms = parts[0].reshape(4, -1)
    return (
        block_out,
        tokens_gradient,
        norms[0],
        norms[1],
        jnp.transpose(sums[0].reshape(input_weight_grad.shape), (1, 0, 2)),
        parts[3],
        parts[4],
        sums[1],
        parts[2],
        norms[2],
        norms[3],
        expand_total,
        parts[5],
        reduce_total,
        parts[1],
    )


def solution(mesh):
    in_specs = (
        P("dp", None),
        P(),
        P(),
        P(None, None, "tensor"),
        P("tensor"),
        P("tensor"),
        P("tensor", None),
        P(),
        P(),
        P(),
        P(None, "tensor"),
        P("tensor"),
        P("tensor", None),
        P(),
        P("dp", None),
    )
    out_specs = (
        P("dp", None),
        P("dp", None),
        P(),
        P(),
        P(None, None, "tensor"),
        P("tensor"),
        P("tensor"),
        P("tensor", None),
        P(),
        P(),
        P(),
        P(None, "tensor"),
        P("tensor"),
        P("tensor", None),
        P(),
    )

    return jax.shard_map(shards, mesh=mesh, in_specs=in_specs, out_specs=out_specs, check_vma=False)
```

```python
import functools

import jax
import jax.numpy as jnp
from jax import lax
from jax.experimental import pallas as pl
from jax.experimental.pallas import tpu as pltpu
from jax.sharding import PartitionSpec as P


HEAD_DIM = 64
PAIR = 2 * HEAD_DIM
F32 = jnp.float32
BF16 = jnp.bfloat16
EXP_SCALE = 0.125 * 1.4426950408889634


norm_eps = 1e-06


def layer_norm(values, gain, shift):
    center = values - jnp.mean(values, axis=-1, keepdims=True)
    spread = jnp.mean(center * center, axis=-1, keepdims=True)
    return center * lax.rsqrt(spread + norm_eps) * gain + shift


def dot_nn(a, b):
    return lax.dot_general(a, b, (((1,), (0,)), ((), ())), preferred_element_type=F32)


def dot_nt(a, b):
    return lax.dot_general(a, b, (((1,), (1,)), ((), ())), preferred_element_type=F32)


def dot_tn(a, b):
    return lax.dot_general(a, b, (((0,), (0,)), ((), ())), preferred_element_type=F32)


def attend_kernel(q_ref, k_ref, v_ref, out_ref, exact_ref, inverse_ref, weights_ref):
    low_half = lax.broadcasted_iota(jnp.int32, (1, PAIR), 1) < HEAD_DIM
    zero = jnp.zeros((), BF16)
    keys, values, queries = k_ref[...], v_ref[...], q_ref[...]
    values = jnp.concatenate([values, jnp.ones_like(values)], axis=1)
    scores = [dot_nt(queries, jnp.where(own, keys, zero)) for own in (low_half, ~low_half)]
    mixed, inverses = [], []
    for head in range(2):
        top = jnp.max(scores[head], axis=1, keepdims=True)
        weights = jnp.exp2((scores[head] - top) * EXP_SCALE).astype(BF16)
        weights_ref[head] = weights
        product = dot_nn(weights, values)
        inverse = 1.0 / product[:, PAIR:]
        mixed.append(product[:, :PAIR] * inverse)
        inverses.append(inverse)
    exact = jnp.where(low_half, mixed[0], mixed[1])
    out_ref[...] = exact.astype(BF16)
    exact_ref[...] = exact
    inverse_ref[...] = jnp.where(low_half, inverses[0], inverses[1])


def attend(queries, keys, values, block=224):
    rows, width = queries.shape
    pairs = width // PAIR
    tile = pl.BlockSpec((block, PAIR), lambda p, i: (i, p))
    whole = pl.BlockSpec((rows, PAIR), lambda p, i: (0, p))
    return pl.pallas_call(
        attend_kernel,
        grid=(pairs, rows // block),
        in_specs=[tile, whole, whole],
        out_specs=[tile, tile, tile, pl.BlockSpec((2, block, rows), lambda p, i: (p, i, 0))],
        out_shape=[
            jax.ShapeDtypeStruct((rows, width), BF16),
            jax.ShapeDtypeStruct((rows, width), F32),
            jax.ShapeDtypeStruct((rows, width), F32),
            jax.ShapeDtypeStruct((2 * pairs, rows, rows), BF16),
        ],
        compiler_params=pltpu.CompilerParams(vmem_limit_bytes=60 << 20),
        cost_estimate=pl.CostEstimate(
            flops=8 * pairs * rows * rows * HEAD_DIM * 4,
            bytes_accessed=4 * pairs * rows * rows,
            transcendentals=2 * pairs * rows * rows,
        ),
        name="attend",
    )(queries, keys, values)


def feed_kernel(n_ref, c_ref, expand_ref, reduce_ref, bias_ref, act_ref, grad_ref, sum_ref, *, chunk):
    @pl.when(pl.program_id(0) == 0)
    def _():
        sum_ref[...] = jnp.zeros_like(sum_ref)

    normed, cotangent = n_ref[...], c_ref[...]
    for first in range(0, expand_ref.shape[1], chunk):
        cols = pl.ds(first, chunk)
        hidden = dot_nn(normed, expand_ref[:, cols]) + bias_ref[:, cols]
        pushed = dot_nt(cotangent, reduce_ref[cols, :])
        share = 0.5 * lax.erf(hidden * ROOT_HALF) + 0.5
        act_ref[:, cols] = (hidden * share).astype(BF16)
        density = jnp.exp2(hidden * hidden * HALF_LOG2E) * NORMAL_PEAK
        grad = (pushed * (share + hidden * density)).astype(BF16)
        grad_ref[:, cols] = grad
        sum_ref[:, cols] += jnp.sum(grad.astype(F32), axis=0, keepdims=True)


def feed(normed, cotangent, expand_weight, reduce_weight, expand_bias, block=224, chunk=256):
    rows, depth = normed.shape
    width = expand_weight.shape[1]
    tile = pl.BlockSpec((block, depth), lambda i: (i, 0))
    out = pl.BlockSpec((block, width), lambda i: (i, 0))

    def whole(shape):
        return pl.BlockSpec(shape, lambda i: (0, 0))

    act, grad, total = pl.pallas_call(
        functools.partial(feed_kernel, chunk=chunk),
        grid=(rows // block,),
        in_specs=[tile, tile, whole((depth, width)), whole((width, depth)), whole((1, width))],
        out_specs=[out, out, whole((1, width))],
        out_shape=[jax.ShapeDtypeStruct((rows, width), BF16)] * 2 + [jax.ShapeDtypeStruct((1, width), F32)],
        compiler_params=pltpu.CompilerParams(vmem_limit_bytes=60 << 20),
        cost_estimate=pl.CostEstimate(
            flops=4 * rows * depth * width, bytes_accessed=8 * rows * (depth + width), transcendentals=rows * width
        ),
        name="feed",
    )(normed, cotangent, expand_weight, reduce_weight, expand_bias.reshape(1, -1))
    return act, grad, total.reshape(-1)


def orders_of(bits):
    if bits == 4:
        return ((0, 1, 2, 3), (1, 0, 2, 3), (2, 0, 1, 3), (2, 1, 0, 3))
    return tuple(tuple((i + j) % bits for j in range(bits)) for i in (0, 1, 2, 3))


class Part:
    def __init__(self, array, first, each, cols, dtype, order, outer):
        self.array, self.first, self.each = array, first, each
        self.cols, self.dtype, self.order, self.outer = cols, dtype, order, outer
        self.inner = order[1:] if outer else order
        self.depth = len(self.inner)
        self.shards = 1 << self.depth
        self.half_rows = self.shards * each


def parts_of(array, shape, dtype, n, shares, orders, outer=True):
    unit = 16 if dtype == BF16 else 8
    units = shape[0] // (n * unit)
    counts = [units * share // sum(shares) for share in shares]
    counts[0] += units - sum(counts)
    parts, first = [], 0
    for count, order in zip(counts, orders):
        if count:
            parts.append(Part(array, first, count * unit, shape[1], dtype, order, outer))
            first += n * count * unit
    return parts


def divides(shape, dtype, n):
    return shape[0] % (n * (16 if dtype == BF16 else 8)) == 0


FEED_PARTS = (
    ((2, 2, 2, 2), ((1, 2, 0, 3), (2, 0, 3, 1), (0, 3, 2, 1), (1, 0, 3, 2))),
    ((2, 1, 1), ((0, 1, 2, 3), (1, 0, 2, 3), (3, 1, 0, 2))),
)
FEED_STEPS = ((2, 0), (5, 0), (0, 0), (1, 0), (5, 1), (4, 0), (3, 0), (1, 1), (2, 1), (6, 0), (3, 1), (4, 1), (5, 2), (2, 2), (1, 2), (0, 1), (0, 2), (1, 3), (5, 3), (6, 1), (3, 2), (4, 2), (6, 2), (3, 3), (1, 4), (6, 3), (0, 3), (6, 4), (4, 3), (2, 3), (2, 4), (3, 4), (1, 5), (4, 4), (6, 5), (0, 4), (5, 4), (2, 5), (0, 5), (3, 5), (4, 5), (5, 5), (3, 6), (6, 6), (1, 6), (4, 6), (5, 6), (0, 6), (2, 6))
FEED_SLOTS = (0, 0, 0, 0, 3, 3, 3, 5, 5, 5, 7, 7, 7, 7, 7, 8, 9, 10, 11, 11, 11, 11, 13, 13, 13, 15, 15, 16, 17, 17, 18, 18, 18, 20, 20, 20, 20, 20, 21, 22, 23, 24, 24, 24, 24, 27, 27, 27, 27)
REST_PARTS = (
    ((2, 2, 4, 2, 2), ((1, 0, 3, 2), (2, 3, 1, 0), (0, 1, 2, 3), (1, 0, 3, 2), (2, 1, 0, 3))),
    ((1, 1), ((0, 2, 1, 3), (1, 0, 3, 2))),
)
REST_STEPS = ((1, 0), (2, 0), (0, 0), (3, 0), (5, 0), (0, 1), (3, 1), (1, 1), (5, 1), (2, 1), (6, 0), (4, 0), (6, 1), (1, 2), (0, 2), (2, 2), (0, 3), (6, 2), (5, 2), (3, 2), (4, 1), (0, 4), (3, 3), (4, 2), (2, 3), (6, 3), (4, 3), (5, 3), (1, 3), (3, 4), (1, 4), (2, 4), (4, 4), (0, 5), (6, 4), (1, 5), (5, 4), (4, 5), (3, 5), (0, 6), (2, 5), (5, 5), (6, 5), (4, 6), (2, 6), (6, 6), (3, 6), (5, 6), (1, 6))


def feed_plan(shapes, n):
    if n == 16:
        parts = [parts_of(i, s, BF16, n, *FEED_PARTS[i]) for i, s in enumerate(shapes)]
        if sum(len(p) for p in parts) == 7:
            return sum(parts, []), FEED_STEPS, FEED_SLOTS
    orders = orders_of(n.bit_length() - 1)
    parts = sum((parts_of(i, s, BF16, n, (1, 1), orders[2 * i : 2 * i + 2]) for i, s in enumerate(shapes)), [])
    steps = [(i, s) for s in range(2 * parts[0].depth + 1) for i in range(len(parts))]
    return parts, steps, None


def rest_plan(shapes, n):
    if n == 16:
        parts = [parts_of(i, s, BF16, n, *REST_PARTS[i]) for i, s in enumerate(shapes)]
        if sum(len(p) for p in parts) == 7:
            return sum(parts, []), REST_STEPS
    orders = orders_of(n.bit_length() - 1)
    parts = sum((parts_of(i, s, BF16, n, (1,), orders[i : i + 1]) for i, s in enumerate(shapes)), [])
    return parts, [(i, s) for s in range(2 * parts[0].depth + 1) for i in range(len(parts))]


def swap_bit(values, bit, n):
    return lax.ppermute(values, "dp", [(j, j ^ (1 << bit)) for j in range(n)])


def bit_of_index(bit):
    return (lax.axis_index("dp") >> bit) & 1


def outer_gift(array, part):
    other = 1 - bit_of_index(part.order[0])
    return lax.dynamic_slice_in_dim(array, part.first + other * part.half_rows, part.half_rows, 0)


def join_kernel(parts, *refs):
    count = len(parts)
    halves, outs = refs[: 2 * count], refs[2 * count : -2 - 4 * count]
    takes, gives = refs[-2 - 4 * count : -2 - 2 * count], refs[-2 - 2 * count : -2]
    take_sem, give_sem = refs[-2:]
    copies = []
    for k in range(2 * count):
        pltpu.make_async_copy(halves[k], takes[k], take_sem.at[k]).start()
    me = lax.axis_index("dp")
    for k in range(2 * count):
        part = parts[k // 2]
        digit = (me // (1 << part.order[0])) % 2
        place = digit if k % 2 == 0 else 1 - digit
        pltpu.make_async_copy(halves[k], takes[k], take_sem.at[k]).wait()
        gives[k][...] = takes[k][...].astype(F32)
        rows = pl.ds(pl.multiple_of(part.first + place * part.half_rows, 8), part.half_rows)
        copies.append(pltpu.make_async_copy(gives[k], outs[part.array].at[rows, :], give_sem.at[k]))
        copies[-1].start()
    for copy in copies:
        copy.wait()


def join(parts, owns, others, shapes):
    halves = [half for pair in zip(owns, others) for half in pair]
    anywhere = pl.BlockSpec(memory_space=pl.ANY)
    takes = [pltpu.VMEM(half.shape, half.dtype) for half in halves]
    gives = [pltpu.VMEM(half.shape, F32) for half in halves]
    size = sum(shape[0] * shape[1] for shape in shapes)
    return pl.pallas_call(
        functools.partial(join_kernel, parts),
        in_specs=[anywhere] * len(halves),
        out_specs=[anywhere] * len(shapes),
        out_shape=[jax.ShapeDtypeStruct(shape, F32) for shape in shapes],
        scratch_shapes=takes
        + gives
        + [pltpu.SemaphoreType.DMA((len(halves),))] * 2,
        compiler_params=pltpu.CompilerParams(vmem_limit_bytes=60 << 20),
        cost_estimate=pl.CostEstimate(flops=size, bytes_accessed=6 * size, transcendentals=0),
        name="join",
    )(*halves)


class Reduction:
    def __init__(self, parts, bits, bufs, lands, gathers, sems):
        self.parts, self.bits = parts, bits
        self.bufs, self.lands, self.gathers = bufs, lands, gathers
        self.load_sem, self.store_sem, self.send_sem, self.recv_sem = sems
        me = lax.axis_index("dp")
        self.digit = [(me // (1 << b)) % 2 for b in range(bits)]
        self.partner = [me + (1 << b) * (1 - 2 * self.digit[b]) for b in range(bits)]

    def greet(self):
        barrier = pltpu.get_barrier_semaphore()
        for b in range(self.bits):
            pl.semaphore_signal(
                barrier, inc=1, device_id={"dp": self.partner[b]}, device_id_type=pl.DeviceIdType.MESH
            )
        pl.semaphore_wait(barrier, self.bits)

    def rows(self, i, position, base=0):
        part, shard = self.parts[i], 0
        for level, b in enumerate(part.inner):
            flip = (position >> (part.depth - 1 - level)) & 1
            shard = shard + (1 << (part.depth - 1 - level)) * ((1 - self.digit[b]) if flip else self.digit[b])
        return pl.ds(pl.multiple_of(base + shard * part.each, 8), part.each)

    def load(self, i, ref, recv):
        part = self.parts[i]
        base = part.first + (self.digit[part.order[0]] * part.half_rows if part.outer else 0)
        for position in range(part.shards):
            pltpu.make_async_copy(
                ref.at[self.rows(i, position, base), :], self.bufs[i].at[position], self.load_sem.at[2 * i]
            ).start()
            if part.outer:
                pltpu.make_async_copy(
                    recv.at[self.rows(i, position), :], self.lands[i].at[position], self.load_sem.at[2 * i + 1]
                ).start()

    def begin(self, i):
        part, buf, land = self.parts[i], self.bufs[i], self.lands[i]
        pltpu.make_async_copy(buf, buf, self.load_sem.at[2 * i]).wait()
        if part.outer:
            got = land.at[pl.ds(0, part.shards)]
            pltpu.make_async_copy(got, got, self.load_sem.at[2 * i + 1]).wait()
            self.add(i, 0, part.shards, buf)

    def add(self, i, start, count, to):
        buf, land = self.bufs[i], self.lands[i]

        def body(j, carry):
            to[j] = (buf[j].astype(F32) + land[start + j].astype(F32)).astype(buf.dtype)
            return carry

        lax.fori_loop(0, count, body, 0)

    def store(self, i, ref):
        base = 0 if self.parts[i].outer else self.parts[i].first
        for position in range(self.parts[i].shards):
            pltpu.make_async_copy(
                self.gathers[i].at[position], ref.at[self.rows(i, position, base), :], self.store_sem.at[i]
            ).start()

    def store_wait(self, i):
        pltpu.make_async_copy(self.gathers[i], self.gathers[i], self.store_sem.at[i]).wait()

    def exchange(self, i, number):
        part = self.parts[i]
        level = number if number < part.depth else 2 * part.depth - 1 - number
        half = part.shards >> (level + 1)
        if number < part.depth:
            at = (part.shards if part.outer else 0) + part.shards - 2 * half
            source, target = self.bufs[i].at[pl.ds(half, half)], self.lands[i].at[pl.ds(at, half)]
        else:
            source, target = self.gathers[i].at[pl.ds(0, half)], self.gathers[i].at[pl.ds(half, half)]
        k = sum(2 * p.depth for p in self.parts[:i]) + number
        return pltpu.make_async_remote_copy(
            source,
            target,
            self.send_sem.at[k],
            self.recv_sem.at[k],
            device_id={"dp": self.partner[part.inner[level]]},
            device_id_type=pl.DeviceIdType.MESH,
        )

    def finish(self, i, number):
        self.exchange(i, number).wait()
        part = self.parts[i]
        if number < part.depth:
            half = part.shards >> (number + 1)
            at = (part.shards if part.outer else 0) + part.shards - 2 * half
            self.add(i, at, half, self.gathers[i] if number == part.depth - 1 else self.bufs[i])


def buffers(summed, gathered):
    return (
        [pltpu.VMEM((p.shards, p.each, p.cols), p.dtype) for p in summed]
        + [pltpu.VMEM((p.shards * (2 if p.outer else 1) - 1, p.each, p.cols), p.dtype) for p in summed]
        + [pltpu.VMEM((p.shards, p.each, p.cols), p.dtype) for p in gathered]
    )


def semaphores(parts):
    exchanges = sum(2 * p.depth for p in parts)
    return [
        pltpu.SemaphoreType.DMA((2 * len(parts),)),
        pltpu.SemaphoreType.DMA((len(parts),)),
        pltpu.SemaphoreType.DMA((exchanges,)),
        pltpu.SemaphoreType.DMA((exchanges,)),
    ]


def attend_back_kernel(parts, plan, slots, bits, arrays, total, *refs):
    count = len(parts)
    q_ref, k_ref, v_ref, o_ref, inverse_ref, weights_ref, branch_ref, ow_ref, att_ref, normed_ref = refs[:10]
    sources, recvs, refs = refs[10 : 10 + arrays], refs[10 + arrays : 10 + arrays + count], refs[10 + arrays + count :]
    dq_ref, dk_ref, dv_ref, dow_ref, diw_ref = refs[:5]
    results, refs = refs[5 : 5 + count], refs[5 + count :]
    dk_sum, dv_sum, g_ref = refs[:3]
    refs = refs[3:]
    sums = Reduction(
        parts, bits, refs[:count], refs[count : 2 * count], refs[2 * count : 3 * count], refs[3 * count :]
    )
    step, steps = pl.program_id(1), pl.num_programs(1)
    low_half = lax.broadcasted_iota(jnp.int32, (1, PAIR), 1) < HEAD_DIM
    zero = jnp.zeros((), BF16)
    now = pl.program_id(0) * steps + step

    @pl.when(now == 0)
    def _():
        for i in range(count):
            sums.load(i, sources[parts[i].array], recvs[i])
        sums.greet()

    def advance(i, number):
        if number == 0:
            sums.begin(i)
        else:
            sums.finish(i, number - 1)
        if number < 2 * parts[i].depth:
            sums.exchange(i, number).start()
        else:
            sums.store(i, results[i])

    places = slots or [total * k // len(plan) for k in range(len(plan))]
    for slot in sorted(set(places)):
        if slot < total:

            @pl.when(now == slot)
            def _(slot=slot):
                for event, place in zip(plan, places):
                    if place == slot:
                        advance(*event)

    @pl.when(step == 0)
    def _():
        dk_sum[...] = jnp.zeros_like(dk_sum)
        dv_sum[...] = jnp.zeros_like(dv_sum)
        branch = branch_ref[...]
        g_ref[...] = dot_nt(branch, ow_ref[...]).astype(BF16)
        dow_ref[...] = dot_tn(att_ref[...], branch).astype(BF16)

    keys, values, queries = k_ref[...], v_ref[...], q_ref[...]
    block = queries.shape[0]
    mine = pl.ds(pl.multiple_of(step * block, block), block)
    grads = (g_ref[mine, :].astype(F32) * inverse_ref[...]).astype(BF16)
    products = grads.astype(F32) * o_ref[...]
    query_grad = None
    for head in range(2):
        own = low_half if head == 0 else ~low_half
        inner = jnp.sum(jnp.where(own, products, 0.0), axis=1, keepdims=True)
        weights = weights_ref[head]
        pushed = dot_nt(grads, jnp.where(own, values, zero))
        score_grad = (weights.astype(F32) * (pushed - inner)).astype(BF16)
        part = dot_nn(score_grad, jnp.where(own, keys, zero))
        query_grad = part if query_grad is None else query_grad + part
        dv_sum[...] += dot_tn(weights, jnp.where(own, grads, zero))
        dk_sum[...] += dot_tn(score_grad, jnp.where(own, queries, zero))
    dq_ref[mine, :] = (query_grad * 0.125).astype(BF16)

    @pl.when(step == steps - 1)
    def _():
        dk_ref[...] = (dk_sum[...] * 0.125).astype(BF16)
        dv_ref[...] = dv_sum[...].astype(BF16)
        joint = jnp.concatenate([dq_ref[...], dk_ref[...], dv_ref[...]], axis=1)
        product = dot_tn(normed_ref[...], joint).astype(BF16)
        for c in range(3):
            diw_ref[c] = product[:, c * PAIR : (c + 1) * PAIR]

    @pl.when(now == total - 1)
    def _():
        for event, place in zip(plan, places):
            if place >= total:
                advance(*event)
        for i in range(count):
            sums.store_wait(i)


def attend_back(queries, keys, values, outs, inverse, weights, branch, output_weight, attended, normed, sources, recvs, plan, bits, block=224):
    parts, plan, slots = plan
    rows, width = queries.shape
    pairs = width // PAIR
    tile = pl.BlockSpec((block, PAIR), lambda p, i: (i, p))
    whole = pl.BlockSpec((rows, PAIR), lambda p, i: (0, p))
    depth = branch.shape[1]
    all_rows = pl.BlockSpec((rows, depth), lambda p, i: (0, 0), pipeline_mode=pl.Buffered(1))
    heads = pl.BlockSpec((PAIR, depth), lambda p, i: (p, 0))
    anywhere = pl.BlockSpec(memory_space=pl.ANY)
    results = pl.pallas_call(
        functools.partial(attend_back_kernel, parts, plan, slots, bits, len(sources), pairs * (rows // block)),
        grid=(pairs, rows // block),
        in_specs=[tile, whole, whole, tile, tile, pl.BlockSpec((2, block, rows), lambda p, i: (p, i, 0))]
        + [all_rows, heads, whole, all_rows]
        + [anywhere] * (len(sources) + len(recvs)),
        out_specs=[whole, whole, whole, heads, pl.BlockSpec((3, depth, PAIR), lambda p, i: (0, 0, p))]
        + [anywhere] * len(parts),
        out_shape=[jax.ShapeDtypeStruct((rows, width), BF16)] * 3
        + [jax.ShapeDtypeStruct((width, depth), BF16), jax.ShapeDtypeStruct((3, depth, width), BF16)]
        + [jax.ShapeDtypeStruct((p.half_rows, p.cols), p.dtype) for p in parts],
        scratch_shapes=[pltpu.VMEM((rows, PAIR), F32)] * 2
        + [pltpu.VMEM((rows, PAIR), BF16)]
        + buffers(parts, parts) + semaphores(parts),
        compiler_params=pltpu.CompilerParams(vmem_limit_bytes=60 << 20, collective_id=0, has_side_effects=True),
        cost_estimate=pl.CostEstimate(
            flops=16 * pairs * rows * rows * HEAD_DIM * 4,
            bytes_accessed=4 * pairs * rows * rows,
            transcendentals=0,
        ),
        name="attend_back",
    )(queries, keys, values, outs, inverse, weights, branch, output_weight, attended, normed, *sources, *recvs)
    return results[:3], results[3], results[4], results[5:]


def rest_kernel(parts, plan, bits, arrays, *refs):
    count = len(parts)
    sources, refs = refs[:arrays], refs[arrays:]
    outer = [i for i, p in enumerate(parts) if p.outer]
    recvs, refs = dict(zip(outer, refs[: len(outer)])), refs[len(outer) :]
    results, refs = refs[:count], refs[count:]
    sums = Reduction(
        parts, bits, refs[:count], refs[count : 2 * count], refs[2 * count : 3 * count], refs[3 * count :]
    )
    for i in range(count):
        sums.load(i, sources[parts[i].array], recvs.get(i))
    sums.greet()

    def advance(i, number):
        if number == 0:
            sums.begin(i)
        else:
            sums.finish(i, number - 1)
        if number < 2 * parts[i].depth:
            sums.exchange(i, number).start()
        else:
            sums.store(i, results[i])

    for event in plan:
        advance(*event)
    for i in range(count):
        sums.store_wait(i)


def rest_sums(sources, recvs, parts, plan, bits):
    anywhere = pl.BlockSpec(memory_space=pl.ANY)
    shapes = [
        jax.ShapeDtypeStruct((p.half_rows if p.outer else p.first + p.shards * p.each, p.cols), p.dtype)
        for p in parts
    ]
    return pl.pallas_call(
        functools.partial(rest_kernel, parts, plan, bits, len(sources)),
        in_specs=[anywhere] * (len(sources) + len(recvs)),
        out_specs=[anywhere] * len(shapes),
        out_shape=shapes,
        scratch_shapes=buffers(parts, parts) + semaphores(parts),
        compiler_params=pltpu.CompilerParams(vmem_limit_bytes=60 << 20, collective_id=1, has_side_effects=True),
        name="rest_sums",
    )(*sources, *recvs)


ROOT_HALF = 0.7071067811865476
HALF_LOG2E = -0.5 * 1.4426950408889634
NORMAL_PEAK = 0.3989422804014327


def column_sum(values):
    return jnp.sum(values, axis=0, dtype=F32)


def shards(
    tokens,
    attention_gain,
    attention_shift,
    input_weight,
    query_bias,
    value_bias,
    output_weight,
    output_bias,
    feedforward_gain,
    feedforward_shift,
    expand_weight,
    expand_bias,
    reduce_weight,
    reduce_bias,
    cotangent,
):
    rows = tokens.shape[0]
    cores = lax.axis_size("tensor")
    core = lax.axis_index("tensor")
    share = rows // cores
    n = lax.axis_size("dp")
    bits = n.bit_length() - 1
    orders = orders_of(bits)

    if cores == 2:

        def own_first(values):
            own = lax.dynamic_slice_in_dim(values, core * share, share, 0)
            return jnp.concatenate([own, lax.dynamic_slice_in_dim(values, (1 - core) * share, share, 0)])

        def swap(values):
            return lax.ppermute(values, "tensor", [(0, 1), (1, 0)])

        def scatter(product, values):
            other = product(*(v[share:] for v in values)).astype(BF16)
            other = swap(other)
            return product(*(v[:share] for v in values)) + other.astype(F32)

        def gather(values):
            return jnp.concatenate([values, swap(values)])

        def gather_in_order(values):
            other = swap(values)
            first = core == 0
            return jnp.concatenate([jnp.where(first, values, other), jnp.where(first, other, values)])

        first_row = 0
    else:

        def own_first(values):
            return values

        def scatter(product, values):
            return lax.psum_scatter(product(*values).astype(BF16), "tensor", scatter_dimension=0, tiled=True).astype(F32)

        def gather(values):
            return lax.all_gather(values, "tensor", axis=0, tiled=True)

        gather_in_order = gather
        first_row = core * share

    def own_rows(values):
        if cores == 2:
            return values[:share]
        return lax.dynamic_slice_in_dim(values, first_row, share, 0)

    stacked_weight = jnp.transpose(input_weight, (1, 0, 2))
    tokens = own_first(tokens)
    cotangent = own_first(cotangent)
    inputs = tokens.astype(F32)
    normed = layer_norm(inputs, attention_gain, attention_shift).astype(BF16)
    queries = (dot_nn(normed, stacked_weight[0]) + query_bias).astype(BF16)
    keys = dot_nn(normed, stacked_weight[1]).astype(BF16)
    values = (dot_nn(normed, stacked_weight[2]) + value_bias).astype(BF16)
    attended, exact, inverse, weights = attend(queries, keys, values)
    own_inputs = own_rows(tokens).astype(F32)
    middle = own_inputs + scatter(lambda part: dot_nn(part, output_weight), (attended,)) + output_bias
    normed_two = layer_norm(middle, feedforward_gain, feedforward_shift).astype(BF16)
    gathered = gather(normed_two)
    activated, hidden_grad, expand_bias_grad = feed(gathered, cotangent, expand_weight, reduce_weight, expand_bias)
    reduce_weight_grad = dot_tn(activated, cotangent).astype(BF16)
    expand_weight_grad = dot_tn(gathered, hidden_grad).astype(BF16)
    feeds = (reduce_weight_grad, expand_weight_grad)
    feed_parts, feed_steps, feed_slots = feed_plan([grad.shape for grad in feeds], n)
    gifts = [outer_gift(feeds[part.array], part) for part in feed_parts]
    hidden_grad, *gifts = lax.optimization_barrier((hidden_grad, *gifts))
    feed_recvs = [swap_bit(gift, part.order[0], n) for gift, part in zip(gifts, feed_parts)]

    normed_two_grad = scatter(lambda part: dot_nt(part, expand_weight), (hidden_grad,))
    own_upstream = own_rows(cotangent).astype(F32)
    _, second_pull = jax.vjp(layer_norm, middle, feedforward_gain, feedforward_shift)
    middle_grad, second_gain_part, second_shift_part = second_pull(normed_two_grad)
    middle_grad = middle_grad + own_upstream
    branch_grad = gather(middle_grad.astype(BF16))
    joint_grad, output_weight_grad, input_weight_grad, feed_sums = attend_back(
        queries,
        keys,
        values,
        exact,
        inverse,
        weights,
        branch_grad,
        output_weight,
        attended,
        normed,
        feeds,
        feed_recvs,
        (feed_parts, feed_steps, feed_slots),
        bits,
    )
    rest = [input_weight_grad.reshape(-1, input_weight_grad.shape[2]), output_weight_grad]
    fits = [divides(part.shape, part.dtype, n) for part in rest]
    sources = [part for part, fit in zip(rest, fits) if fit]
    rest_parts, rest_steps = rest_plan([part.shape for part in sources], n)
    gifts = [outer_gift(sources[part.array], part) for part in rest_parts]
    *joint_grad, activated, feed_sums, gifts = lax.optimization_barrier((*joint_grad, activated, feed_sums, gifts))
    rest_recvs = [swap_bit(gift, part.order[0], n) for gift, part in zip(gifts, rest_parts)]
    feed_others = [swap_bit(own, part.order[0], n) for own, part in zip(feed_sums, feed_parts)]

    def back_through(query_part, key_part, value_part):
        return (
            dot_nt(query_part, stacked_weight[0])
            + dot_nt(key_part, stacked_weight[1])
            + dot_nt(value_part, stacked_weight[2])
        )

    normed_grad = scatter(back_through, tuple(joint_grad))
    _, first_pull = jax.vjp(layer_norm, own_inputs, attention_gain, attention_shift)
    inputs_grad, first_gain_part, first_shift_part = first_pull(normed_grad)
    tokens_gradient = gather_in_order((inputs_grad + middle_grad).astype(BF16))
    update = scatter(lambda part: dot_nn(part, reduce_weight), (activated,))
    result = middle + (update + reduce_bias)
    block_out = gather_in_order(result.astype(BF16))
    norm_parts = jnp.stack([first_gain_part, first_shift_part, second_gain_part, second_shift_part])
    norm_parts = norm_parts + swap(norm_parts) if cores == 2 else lax.psum(norm_parts, "tensor")
    small = [
        norm_parts.reshape(-1),
        column_sum(cotangent),
        column_sum(branch_grad),
        column_sum(joint_grad[0]),
        column_sum(joint_grad[2]),
        expand_bias_grad,
    ]
    sizes = [part.shape[0] for part in small]
    table_rows = -(-sum(sizes) // (n * 8 * 128)) * n * 8
    table = jnp.pad(jnp.concatenate(small), (0, table_rows * 128 - sum(sizes))).reshape(table_rows, 128)
    table_parts = parts_of(len(sources), table.shape, F32, n, (1,), orders, outer=False)
    steps = list(rest_steps)
    for k in range(2 * bits, -1, -1):
        steps.insert(k * len(steps) // (2 * bits + 1), (len(rest_parts), k))
    summed = rest_sums([*sources, table], rest_recvs, rest_parts + table_parts, steps, bits)
    rest_others = [swap_bit(own, part.order[0], n) for own, part in zip(summed, rest_parts)]
    feed_sums, summed = lax.optimization_barrier((feed_sums, summed))
    reduce_total, expand_total = join(feed_parts, feed_sums, feed_others, [grad.shape for grad in feeds])
    joined = list(join(rest_parts, summed[:-1], rest_others, [part.shape for part in sources]))
    sums = [joined.pop(0) if fit else lax.psum(part, "dp").astype(F32) for part, fit in zip(rest, fits)]
    flat = summed[-1].reshape(-1)
    ends = [sum(sizes[: i + 1]) for i in range(len(sizes))]
    parts = [flat[end - size : end] for size, end in zip(sizes, ends)]
    norms = parts[0].reshape(4, -1)
    return (
        block_out,
        tokens_gradient,
        norms[0],
        norms[1],
        jnp.transpose(sums[0].reshape(input_weight_grad.shape), (1, 0, 2)),
        parts[3],
        parts[4],
        sums[1],
        parts[2],
        norms[2],
        norms[3],
        expand_total,
        parts[5],
        reduce_total,
        parts[1],
    )


def solution(mesh):
    in_specs = (
        P("dp", None),
        P(),
        P(),
        P(None, None, "tensor"),
        P("tensor"),
        P("tensor"),
        P("tensor", None),
        P(),
        P(),
        P(),
        P(None, "tensor"),
        P("tensor"),
        P("tensor", None),
        P(),
        P("dp", None),
    )
    out_specs = (
        P("dp", None),
        P("dp", None),
        P(),
        P(),
        P(None, None, "tensor"),
        P("tensor"),
        P("tensor"),
        P("tensor", None),
        P(),
        P(),
        P(),
        P(None, "tensor"),
        P("tensor"),
        P("tensor", None),
        P(),
    )

    return jax.shard_map(shards, mesh=mesh, in_specs=in_specs, out_specs=out_specs, check_vma=False)
```
